8 devices in a mesh: col: 2 (over z, y), row: 4 (over x, core).
Axes of the slice: x: 2, y: 2, z: 1, core: 2. Of those that a mesh axis runs over, the one named last changes fastest.
Arguments:
- img_emb: bfloat16 [8192, 512], P(('row', 'col'))
- txt_emb: bfloat16 [8192, 512], P(('row', 'col'))
- log_scale: float32 [], replicated
Outputs:
- output 1: float32 [], replicated
- output 2: bfloat16 [8192, 512], P(('row', 'col'))
- output 3: bfloat16 [8192, 512], P(('row', 'col'))
- output 4: float32 [], replicated
All inputs are finite; a program needn't handle non-finite values.
Results may differ from the reference program's by a relative error of at most 0.001.
Values are sent between devices in bfloat16 or wider.
A program may use at most 1 GiB of HBM per device.

```python
import jax
import jax.numpy as jnp
from jax import lax

ROWS_DEV = 1024
SHARDS = 8
EMBED_DIM = 512
BATCH = ROWS_DEV * SHARDS


def unit_rows(values):
    return values / jnp.sqrt(jnp.sum(values * values, axis=-1, keepdims=True))


def setup_inputs(seed: int = 0) -> dict:
    keys = jax.random.split(jax.random.key(seed), 5)
    shared_dir = unit_rows(jax.random.normal(keys[0], (EMBED_DIM,), jnp.float32))
    spread = (1.0 / EMBED_DIM) ** 0.5
    pair_part = jax.random.normal(keys[1], (BATCH, EMBED_DIM), jnp.float32) * spread
    noise_img = jax.random.normal(keys[2], (BATCH, EMBED_DIM), jnp.float32) * spread
    noise_txt = jax.random.normal(keys[3], (BATCH, EMBED_DIM), jnp.float32) * spread
    img_emb = unit_rows(0.7 * shared_dir + 0.5 * pair_part + 0.5 * noise_img)
    txt_emb = unit_rows(0.7 * shared_dir + 0.5 * pair_part + 0.5 * noise_txt)
    log_scale = jnp.log(jax.random.uniform(keys[4], (), jnp.float32, 10.0, 30.0))
    return {"img_emb": img_emb.astype(jnp.bfloat16), "txt_emb": txt_emb.astype(jnp.bfloat16), "log_scale": log_scale}


def reference(img_emb, txt_emb, log_scale):
    logit_scale = jnp.exp(log_scale)
    img_blocks = img_emb.reshape(SHARDS, ROWS_DEV, EMBED_DIM)
    txt_blocks = txt_emb.reshape(SHARDS, ROWS_DEV, EMBED_DIM)
    block_ids = jnp.arange(SHARDS)
    positions = jnp.arange(BATCH)
    inv_count = 1.0 / (2 * BATCH)

    def row_lse_of(img_block):
        logits = logit_scale * jnp.dot(img_block, txt_emb.T, preferred_element_type=jnp.float32)
        return jax.nn.logsumexp(logits, axis=1)

    def col_lse_of(txt_block):
        logits_t = logit_scale * jnp.dot(txt_block, img_emb.T, preferred_element_type=jnp.float32)
        return jax.nn.logsumexp(logits_t, axis=1)

    row_lse = lax.map(row_lse_of, img_blocks).reshape(BATCH)
    col_lse = lax.map(col_lse_of, txt_blocks).reshape(BATCH)
    pos_logits = logit_scale * jnp.sum(img_emb.astype(jnp.float32) * txt_emb.astype(jnp.float32), axis=1)
    total_loss = (jnp.sum(row_lse - pos_logits) + jnp.sum(col_lse - pos_logits)) * inv_count

    def img_grad_of(block_args):
        block_id, img_block, row_lse_blk = block_args
        logits = logit_scale * jnp.dot(img_block, txt_emb.T, preferred_element_type=jnp.float32)
        diag_mask = (block_id * ROWS_DEV + jnp.arange(ROWS_DEV))[:, None] == positions[None, :]
        grad_tile = (jnp.exp(logits - row_lse_blk[:, None]) + jnp.exp(logits - col_lse[None, :]) - jnp.where(diag_mask, 2.0, 0.0)) * inv_count
        d_block = logit_scale * jnp.dot(grad_tile.astype(jnp.bfloat16), txt_emb, preferred_element_type=jnp.float32)
        return d_block.astype(jnp.bfloat16), jnp.sum(grad_tile * logits)

    def txt_grad_of(block_args):
        block_id, txt_block, col_lse_blk = block_args
        logits_t = logit_scale * jnp.dot(txt_block, img_emb.T, preferred_element_type=jnp.float32)
        diag_mask = (block_id * ROWS_DEV + jnp.arange(ROWS_DEV))[:, None] == positions[None, :]
        grad_t = (jnp.exp(logits_t - row_lse[None, :]) + jnp.exp(logits_t - col_lse_blk[:, None]) - jnp.where(diag_mask, 2.0, 0.0)) * inv_count
        d_block = logit_scale * jnp.dot(grad_t.astype(jnp.bfloat16), img_emb, preferred_element_type=jnp.float32)
        return d_block.astype(jnp.bfloat16)

    d_img, dt_parts = lax.map(img_grad_of, (block_ids, img_blocks, row_lse.reshape(SHARDS, ROWS_DEV)))
    d_txt = lax.map(txt_grad_of, (block_ids, txt_blocks, col_lse.reshape(SHARDS, ROWS_DEV)))
    return total_loss, d_img.reshape(BATCH, EMBED_DIM), d_txt.reshape(BATCH, EMBED_DIM), jnp.sum(dt_parts)
```

```python
import functools
import math

import jax
import jax.numpy as jnp
from jax import lax
from jax.experimental import pallas as pl
from jax.experimental.pallas import tpu as pltpu
from jax.sharding import PartitionSpec as P

MESH = pl.DeviceIdType.MESH
F32 = jnp.float32
BF16 = jnp.bfloat16
ROWS = 1024
DIM = 512
CHUNK = 256
STEPS = ROWS // CHUNK
IMGS = 2 * ROWS
TXTS = 4 * ROWS
LOG2E = math.log2(math.e)


def kernel(inv_count, scale_ref, img_hbm, txt_hbm, loss_ref, dimg_hbm, dtxt_hbm, dscale_ref,
           img, txt, exps, row_e, row_m, col_e, col_m, row_send, row_recv, col_send, col_recv, col_b,
           g_row, g_col, d_img_send, d_img_recv, d_img_own, ring, d_txt_x, d_txt_p, d_txt_recv, d_txt_own, out_stage,
           scal, scal_y, load_sem, gy_send, gy_recv, gx_send, gx_recv, gp_sem, gf_send, gf_recv, row_sem, col_ssem, col_rsem,
           ry_send, ry_recv, rp_send, rp_recv, rx_send, rx_recv, sc_ssem, sc_rsem, out_sem):
    row = lax.axis_index("row")
    col = lax.axis_index("col")
    core = lax.rem(row, 2)
    partner = row + 1 - 2 * core
    across = lax.rem(row + 2, 4)
    diagonal = across + 1 - 2 * core
    peers = (partner, across, diagonal)
    other_col = 1 - col

    def to_y(src, dst, ssem, rsem):
        return pltpu.make_async_remote_copy(src, dst, ssem, rsem, device_id={"row": row, "col": other_col}, device_id_type=MESH)

    def to_row(src, dst, ssem, rsem, peer):
        return pltpu.make_async_remote_copy(src, dst, ssem, rsem, device_id={"row": peer, "col": col}, device_id_type=MESH)

    load_img = pltpu.make_async_copy(img_hbm, img.at[pl.ds(0, ROWS)], load_sem.at[0])
    load_txt = pltpu.make_async_copy(txt_hbm, txt.at[pl.ds(0, ROWS)], load_sem.at[1])
    load_img.start()
    load_txt.start()

    barrier = pltpu.get_barrier_semaphore()
    for peer in peers:
        pl.semaphore_signal(barrier, inc=1, device_id={"row": peer, "col": col}, device_id_type=MESH)
    pl.semaphore_signal(barrier, inc=1, device_id={"row": row, "col": other_col}, device_id_type=MESH)

    scale = jnp.max(jnp.exp(jnp.full((8, 128), scale_ref[0, 0], F32)))
    scale2 = scale * LOG2E
    row_e[...] = jnp.zeros_like(row_e)
    row_m[...] = jnp.zeros_like(row_m)
    col_e[...] = jnp.zeros_like(col_e)
    col_m[...] = jnp.zeros_like(col_m)

    load_img.wait()
    load_txt.wait()
    pl.semaphore_wait(barrier, 4)

    gather_y, gather_x = [], []
    for k in range(STEPS):
        part = pl.ds(k * CHUNK, CHUNK)
        gather_x.append(to_row(txt.at[part], txt.at[pl.ds(2 * ROWS + k * CHUNK, CHUNK)], gx_send.at[k], gx_recv.at[k], across))
        gather_y.append(to_y(img.at[part], img.at[pl.ds(ROWS + k * CHUNK, CHUNK)], gy_send.at[k], gy_recv.at[k]))
        gather_x[k].start()
        gather_y[k].start()
    gather_p = to_row(txt.at[pl.ds(0, ROWS)], txt.at[pl.ds(ROWS, ROWS)], gp_sem.at[0], gp_sem.at[1], partner)
    gather_p.start()
    relay = [
        to_row(txt.at[pl.ds(2 * ROWS + k * CHUNK, CHUNK)], txt.at[pl.ds(3 * ROWS + k * CHUNK, CHUNK)], gf_send.at[k], gf_recv.at[k], partner)
        for k in range(STEPS)
    ]

    def logit_block(r0, nr, c0, nc):
        rows = pl.ds(r0, nr)
        cols = pl.ds(c0, nc)
        dots = lax.dot_general(img[rows, :], txt[cols, :], (((1,), (1,)), ((), ())), preferred_element_type=F32)
        e = jnp.exp2(dots * scale2)
        exps[rows, cols] = e
        m = e * dots
        for values, row_sum, col_sum in ((e, row_e, col_e), (m, row_m, col_m)):
            acc = values[:, 0:128]
            for q in range(1, nc // 128):
                acc = acc + values[:, q * 128:(q + 1) * 128]
            row_sum[rows, :] += acc
            col_sum[:, cols] += jnp.sum(values.reshape(nr // 8, 8, nc), axis=0)

    def own_rows(c0):
        def body(i, carry):
            logit_block(pl.multiple_of(i * 512, 512), 512, c0, CHUNK)
            return carry
        lax.fori_loop(0, 2, body, 0)

    def sweep_cols(r0, c0, n):
        if n == 0:
            return
        def body(i, carry):
            logit_block(r0, CHUNK, pl.multiple_of(c0 + i * CHUNK, CHUNK), CHUNK)
            return carry
        lax.fori_loop(0, n, body, 0)

    def sweep_rows(r0, c0, n):
        if n == 0:
            return
        def body(i, carry):
            logit_block(pl.multiple_of(r0 + i * CHUNK, CHUNK), CHUNK, c0, CHUNK)
            return carry
        lax.fori_loop(0, n, body, 0)

    def four_cols(c0):
        def body(i, carry):
            own_rows(pl.multiple_of(c0 + i * CHUNK, CHUNK))
            return carry
        lax.fori_loop(0, STEPS, body, 0)

    four_cols(0)

    def diag_body(i, acc):
        part = pl.ds(pl.multiple_of(i * 128, 128), 128)
        prod = img[part, :].astype(F32) * txt[part, :].astype(F32)
        return acc + jnp.sum(prod.reshape(16, 8, DIM), axis=0)
    diag_sum = jnp.sum(lax.fori_loop(0, 8, diag_body, jnp.zeros((8, DIM), F32)))

    gather_p.wait_recv()
    four_cols(ROWS)
    for k in range(STEPS):
        new_row = ROWS + k * CHUNK
        gather_x[k].wait_recv()
        relay[k].start()
        own_rows(2 * ROWS + k * CHUNK)
        gather_y[k].wait_recv()
        sweep_cols(new_row, 0, 2 * STEPS)
        sweep_cols(new_row, 2 * ROWS, k + 1)
        sweep_rows(ROWS, 2 * ROWS + k * CHUNK, k)
        relay[k].wait_recv()
        own_rows(3 * ROWS + k * CHUNK)
        sweep_cols(new_row, 3 * ROWS, k + 1)
        sweep_rows(ROWS, 3 * ROWS + k * CHUNK, k)

    row_send[...] = jnp.sum(row_e[...].T, axis=0, keepdims=True)
    col_send[...] = jnp.sum(col_e[...], axis=0, keepdims=True)
    swap_row = to_y(row_send, row_recv, row_sem.at[0], row_sem.at[1])
    swap_row.start()
    swap_col = []
    for t, peer in enumerate(peers):
        swap_col.append(to_row(col_send, col_recv.at[t], col_ssem.at[t], col_rsem.at[t], peer))
        swap_col[t].start()
    swap_row.wait_recv()
    row_tot = row_send[...] + jnp.concatenate([row_recv[:, ROWS:], row_recv[:, :ROWS]], axis=1)
    row_a = row_e
    row_a[...] = jnp.broadcast_to(inv_count / row_tot, (128, IMGS)).T
    for t in range(3):
        swap_col[t].wait_recv()
    def slot(ref, s):
        return ref[:, s * ROWS:(s + 1) * ROWS]
    col_tots = []
    for s in range(4):
        tot = (slot(col_send, s) + slot(col_recv.at[0], s ^ 1)) + (slot(col_recv.at[1], s ^ 2) + slot(col_recv.at[2], s ^ 3))
        col_b[:, s * ROWS:(s + 1) * ROWS] = inv_count / tot
        col_tots.append(tot)

    def d_img_chunk(r0):
        rows = pl.ds(r0, CHUNK)
        def body(j, carry):
            for q in range(4):
                cols = pl.ds(pl.multiple_of(j * 512, 512) + q * 128, 128)
                g_row[:, cols] = (exps[rows, cols] * (row_a[rows, :] + col_b[:, cols])).astype(BF16)
            return carry
        lax.fori_loop(0, TXTS // 512, body, 0)
        return jnp.dot(g_row[...], txt[...], preferred_element_type=F32)

    def d_txt_chunk(c0):
        def body(i, carry):
            rows = pl.ds(pl.multiple_of(i * CHUNK, CHUNK), CHUNK)
            for q in range(CHUNK // 128):
                cols = pl.ds(c0 + q * 128, 128)
                g_col[rows, q * 128:(q + 1) * 128] = (exps[rows, cols] * (row_a[rows, :] + col_b[:, cols])).astype(BF16)
            return carry
        lax.fori_loop(0, IMGS // CHUNK, body, 0)
        return lax.dot_general(g_col[...], img[...], (((0,), (0,)), ((), ())), preferred_element_type=F32)

    send_y, send_p, send_x = [], [], []
    for k in range(STEPS):
        part = pl.ds(k * CHUNK, CHUNK)
        d_img_send[part, :] = d_img_chunk(ROWS + k * CHUNK)
        send_y.append(to_y(d_img_send.at[part], d_img_recv.at[part], ry_send.at[k], ry_recv.at[k]))
        send_y[k].start()
        if k >= 2:
            send_p[k - 2].wait_send()
        ring[k % 2] = d_txt_chunk(3 * ROWS + k * CHUNK)
        send_p.append(to_row(ring.at[k % 2], d_txt_x.at[part], rp_send.at[k], rp_recv.at[k], partner))
        send_p[k].start()
        mine = d_txt_chunk(2 * ROWS + k * CHUNK)
        send_p[k].wait_recv()
        d_txt_x[part, :] += mine
        send_x.append(to_row(d_txt_x.at[part], d_txt_recv.at[part], rx_send.at[k], rx_recv.at[k], across))
        send_x[k].start()

    own_r = row_send[:, :ROWS] + row_recv[:, ROWS:]
    loss_part = jnp.sum(jnp.log(own_r) + jnp.log(col_tots[0])) - 2.0 * scale * diag_sum
    dscale_part = scale * (jnp.sum(row_a[...] * row_m[...]) + jnp.sum(jnp.sum(col_m[...], axis=0, keepdims=True) * col_b[...])
                           - 2.0 * inv_count * diag_sum)
    lane = lax.broadcasted_iota(jnp.int32, (8, 128), 1)
    scal[0] = jnp.where(lane == 0, loss_part * inv_count, dscale_part)
    send_s = []
    for t, peer in enumerate(peers):
        send_s.append(to_row(scal.at[0], scal.at[t + 1], sc_ssem.at[t], sc_rsem.at[t], peer))
        send_s[t].start()

    def fix_body(i, carry):
        part = pl.ds(pl.multiple_of(i * 128, 128), 128)
        on_diag = lax.broadcasted_iota(jnp.int32, (128, 128), 0) == lax.broadcasted_iota(jnp.int32, (128, 128), 1)
        term = (2.0 * inv_count) / (row_a[part, :] + col_b[:, part])
        exps[part, part] = exps[part, part] - jnp.where(on_diag, term, 0.0)
        return carry
    lax.fori_loop(0, ROWS // 128, fix_body, 0)

    for k in range(STEPS):
        part = pl.ds(k * CHUNK, CHUNK)
        send_p[STEPS + k - 2].wait_send()
        ring[k % 2] = d_txt_chunk(ROWS + k * CHUNK)
        send_p.append(to_row(ring.at[k % 2], d_txt_p.at[part], rp_send.at[STEPS + k], rp_recv.at[STEPS + k], partner))
        send_p[STEPS + k].start()

    for t in range(3):
        send_s[t].wait_recv()
    scal_y[0] = (scal[0] + scal[1]) + (scal[2] + scal[3])
    swap_s = to_y(scal_y.at[0], scal_y.at[1], sc_ssem.at[3], sc_rsem.at[3])
    swap_s.start()

    outs = []
    for k in range(STEPS):
        part = pl.ds(k * CHUNK, CHUNK)
        slot_k = k % 2
        d_img_own[...] = d_img_chunk(k * CHUNK)
        d_txt_own[...] = d_txt_chunk(k * CHUNK)
        send_p[STEPS + k].wait_recv()
        d_txt_own[...] += d_txt_p[part, :]
        if k >= 2:
            outs[2 * k - 4].wait()
            outs[2 * k - 3].wait()
        send_y[k].wait_recv()
        out_stage[slot_k, 0] = (scale * (d_img_own[...] + d_img_recv[part, :])).astype(BF16)
        outs.append(pltpu.make_async_copy(out_stage.at[slot_k, 0], dimg_hbm.at[part], out_sem.at[2 * k]))
        outs[2 * k].start()
        send_x[k].wait_recv()
        out_stage[slot_k, 1] = (scale * (d_txt_own[...] + d_txt_recv[part, :])).astype(BF16)
        outs.append(pltpu.make_async_copy(out_stage.at[slot_k, 1], dtxt_hbm.at[part], out_sem.at[2 * k + 1]))
        outs[2 * k + 1].start()

    swap_s.wait_recv()
    total = scal_y[0] + scal_y[1]
    loss_ref[0, 0] = total[0, 0]
    dscale_ref[0, 0] = total[0, 1]

    for k in range(STEPS):
        gather_x[k].wait_send()
        gather_y[k].wait_send()
        relay[k].wait_send()
        send_y[k].wait_send()
        send_x[k].wait_send()
    gather_p.wait_send()
    swap_row.wait_send()
    for t in range(3):
        swap_col[t].wait_send()
        send_s[t].wait_send()
    swap_s.wait_send()
    for k in range(2 * STEPS - 2, 2 * STEPS):
        send_p[k].wait_send()
    for k in range(2 * STEPS - 4, 2 * STEPS):
        outs[k].wait()


def solution(mesh):
    batch_spec = P(("row", "col"), None)
    n_dev = mesh.shape["row"] * mesh.shape["col"]
    inv_count = 1.0 / (2 * ROWS * n_dev)
    dma = pltpu.SemaphoreType.DMA

    def local_tile(img_loc, txt_loc, log_scale):
        any_spec = pl.BlockSpec(memory_space=pl.ANY)
        smem_spec = pl.BlockSpec(memory_space=pltpu.SMEM)
        loss, d_img, d_txt, d_scale = pl.pallas_call(
            functools.partial(kernel, inv_count),
            out_shape=(
                jax.ShapeDtypeStruct((1, 1), F32),
                jax.ShapeDtypeStruct((ROWS, DIM), BF16),
                jax.ShapeDtypeStruct((ROWS, DIM), BF16),
                jax.ShapeDtypeStruct((1, 1), F32),
            ),
            in_specs=[smem_spec, any_spec, any_spec],
            out_specs=(smem_spec, any_spec, any_spec, smem_spec),
            scratch_shapes=[
                pltpu.VMEM((IMGS, DIM), BF16),
                pltpu.VMEM((TXTS, DIM), BF16),
                pltpu.VMEM((IMGS, TXTS), F32),
                pltpu.VMEM((IMGS, 128), F32),
                pltpu.VMEM((IMGS, 128), F32),
                pltpu.VMEM((8, TXTS), F32),
                pltpu.VMEM((8, TXTS), F32),
                pltpu.VMEM((1, IMGS), F32),
                pltpu.VMEM((1, IMGS), F32),
                pltpu.VMEM((1, TXTS), F32),
                pltpu.VMEM((3, 1, TXTS), F32),
                pltpu.VMEM((1, TXTS), F32),
                pltpu.VMEM((CHUNK, TXTS), BF16),
                pltpu.VMEM((IMGS, CHUNK), BF16),
                pltpu.VMEM((ROWS, DIM), F32),
                pltpu.VMEM((ROWS, DIM), F32),
                pltpu.VMEM((CHUNK, DIM), F32),
                pltpu.VMEM((2, CHUNK, DIM), F32),
                pltpu.VMEM((ROWS, DIM), F32),
                pltpu.VMEM((ROWS, DIM), F32),
                pltpu.VMEM((ROWS, DIM), F32),
                pltpu.VMEM((CHUNK, DIM), F32),
                pltpu.VMEM((2, 2, CHUNK, DIM), BF16),
                pltpu.VMEM((4, 8, 128), F32),
                pltpu.VMEM((2, 8, 128), F32),
                dma((2,)),
                dma((STEPS,)), dma((STEPS,)),
                dma((STEPS,)), dma((STEPS,)),
                dma((2,)),
                dma((STEPS,)), dma((STEPS,)),
                dma((2,)),
                dma((3,)), dma((3,)),
                dma((STEPS,)), dma((STEPS,)),
                dma((2 * STEPS,)), dma((2 * STEPS,)),
                dma((STEPS,)), dma((STEPS,)),
                dma((4,)), dma((4,)),
                dma((2 * STEPS,)),
            ],
            compiler_params=pltpu.CompilerParams(
                collective_id=0, has_side_effects=True, vmem_limit_bytes=67043328,
            ),
            name="clip_loss",
        )(log_scale.reshape(1, 1), img_loc, txt_loc)
        return loss.reshape(()), d_img, d_txt, d_scale.reshape(())

    return jax.shard_map(local_tile, mesh=mesh, in_specs=(batch_spec, batch_spec, P()), out_specs=(P(), batch_spec, batch_spec, P()), check_vma=False)
```

```python
import functools
import math

import jax
import jax.numpy as jnp
from jax import lax
from jax.experimental import pallas as pl
from jax.experimental.pallas import tpu as pltpu
from jax.sharding import PartitionSpec as P

MESH = pl.DeviceIdType.MESH
F32 = jnp.float32
BF16 = jnp.bfloat16
ROWS = 1024
DIM = 512
CHUNK = 256
STEPS = ROWS // CHUNK
IMGS = 2 * ROWS
TXTS = 4 * ROWS
X_BASE = 2 * ROWS
LOG2E = math.log2(math.e)


def kernel(inv_count, scale_ref, img_hbm, txt_hbm, loss_ref, dimg_hbm, dtxt_hbm, dscale_ref,
           img, txt, exps, row_e, row_m, col_e, col_m, row_send, row_recv, col_send, col_recv, col_b,
           d_img_send, d_img_recv, d_img_own, ring, d_txt_x, d_txt_p, d_txt_recv, out_stage,
           scal, scal_y, load_sem, gy_send, gy_recv, gx_send, gx_recv, gp_sem, gf_send, gf_recv, row_sem, col_ssem, col_rsem,
           ry_send, ry_recv, rp_send, rp_recv, rx_send, rx_recv, sc_ssem, sc_rsem, out_sem):
    row = lax.axis_index("row")
    col = lax.axis_index("col")
    core = lax.rem(row, 2)
    partner = row + 1 - 2 * core
    across = lax.rem(row + 2, 4)
    diagonal = across + 1 - 2 * core
    peers = (partner, across, diagonal)
    other_col = 1 - col

    def to_y(src, dst, ssem, rsem):
        return pltpu.make_async_remote_copy(src, dst, ssem, rsem, device_id={"row": row, "col": other_col}, device_id_type=MESH)

    def to_row(src, dst, ssem, rsem, peer):
        return pltpu.make_async_remote_copy(src, dst, ssem, rsem, device_id={"row": peer, "col": col}, device_id_type=MESH)

    load_img = pltpu.make_async_copy(img_hbm, img.at[pl.ds(0, ROWS)], load_sem.at[0])
    load_txt = pltpu.make_async_copy(txt_hbm, txt.at[pl.ds(0, ROWS)], load_sem.at[1])
    load_img.start()
    load_txt.start()

    barrier = pltpu.get_barrier_semaphore()
    for peer in peers:
        pl.semaphore_signal(barrier, inc=1, device_id={"row": peer, "col": col}, device_id_type=MESH)
    pl.semaphore_signal(barrier, inc=1, device_id={"row": row, "col": other_col}, device_id_type=MESH)

    scale = jnp.max(jnp.exp(jnp.full((8, 128), scale_ref[0, 0], F32)))
    scale2 = scale * LOG2E
    row_e[...] = jnp.zeros_like(row_e)
    row_m[...] = jnp.zeros_like(row_m)
    col_e[...] = jnp.zeros_like(col_e)
    col_m[...] = jnp.zeros_like(col_m)

    load_img.wait()
    load_txt.wait()
    pl.semaphore_wait(barrier, 4)

    gather_y, gather_x = [], []
    for k in range(STEPS):
        part = pl.ds(k * CHUNK, CHUNK)
        gather_x.append(to_row(txt.at[part], txt.at[pl.ds(X_BASE + 2 * k * CHUNK, CHUNK)], gx_send.at[k], gx_recv.at[k], across))
        gather_y.append(to_y(img.at[part], img.at[pl.ds(ROWS + k * CHUNK, CHUNK)], gy_send.at[k], gy_recv.at[k]))
        gather_x[k].start()
        gather_y[k].start()
    gather_p = to_row(txt.at[pl.ds(0, ROWS)], txt.at[pl.ds(ROWS, ROWS)], gp_sem.at[0], gp_sem.at[1], partner)
    gather_p.start()
    relay = [
        to_row(txt.at[pl.ds(X_BASE + 2 * k * CHUNK, CHUNK)], txt.at[pl.ds(X_BASE + (2 * k + 1) * CHUNK, CHUNK)], gf_send.at[k], gf_recv.at[k], partner)
        for k in range(STEPS)
    ]

    def logit_block(r0, nr, c0, nc):
        rows = pl.ds(r0, nr)
        cols = pl.ds(c0, nc)
        dots = lax.dot_general(img[rows, :], txt[cols, :], (((1,), (1,)), ((), ())), preferred_element_type=F32)
        e = jnp.exp2(dots * scale2)
        exps[rows, cols] = e
        m = e * dots
        for values, row_sum, col_sum in ((e, row_e, col_e), (m, row_m, col_m)):
            acc = values[:, 0:128]
            for q in range(1, nc // 128):
                acc = acc + values[:, q * 128:(q + 1) * 128]
            row_sum[rows, :] += acc
            col_sum[:, cols] += jnp.sum(values.reshape(nr // 8, 8, nc), axis=0)

    def own_by_own(i, carry):
        logit_block(0, ROWS, pl.multiple_of(i * 512, 512), 512)
        return carry

    lax.fori_loop(0, 2, own_by_own, 0)

    def diag_body(i, acc):
        part = pl.ds(pl.multiple_of(i * 128, 128), 128)
        prod = img[part, :].astype(F32) * txt[part, :].astype(F32)
        return acc + jnp.sum(prod.reshape(16, 8, DIM), axis=0)
    diag_sum = jnp.sum(lax.fori_loop(0, 8, diag_body, jnp.zeros((8, DIM), F32)))

    gather_p.wait_recv()
    lax.fori_loop(2, 4, own_by_own, 0)
    for k in range(STEPS):
        new_row = ROWS + k * CHUNK
        gather_x[k].wait_recv()
        relay[k].start()
        gather_y[k].wait_recv()
        def new_by_held(i, carry, new_row=new_row):
            logit_block(new_row, CHUNK, pl.multiple_of(i * 512, 512), 512)
            return carry
        lax.fori_loop(0, 4 + k, new_by_held, 0)
        relay[k].wait_recv()
        logit_block(0, ROWS, X_BASE + 2 * k * CHUNK, 2 * CHUNK)
        logit_block(ROWS, (k + 1) * CHUNK, X_BASE + 2 * k * CHUNK, 2 * CHUNK)

    row_send[...] = jnp.sum(row_e[...].T, axis=0, keepdims=True)
    col_send[...] = jnp.sum(col_e[...], axis=0, keepdims=True)
    swap_row = to_y(row_send, row_recv, row_sem.at[0], row_sem.at[1])
    swap_row.start()
    swap_col = []
    for t, peer in enumerate(peers):
        swap_col.append(to_row(col_send, col_recv.at[t], col_ssem.at[t], col_rsem.at[t], peer))
        swap_col[t].start()
    swap_row.wait_recv()
    row_tot = row_send[...] + jnp.concatenate([row_recv[:, ROWS:], row_recv[:, :ROWS]], axis=1)
    row_a = row_e
    row_a[...] = jnp.broadcast_to(inv_count / row_tot, (128, IMGS)).T
    for t in range(3):
        swap_col[t].wait_recv()
    def slot(ref, s):
        if s < 2:
            return ref[:, s * ROWS:(s + 1) * ROWS]
        starts = [X_BASE + (2 * k + s - 2) * CHUNK for k in range(STEPS)]
        return jnp.concatenate([ref[:, c:c + CHUNK] for c in starts], axis=1)
    for s in range(4):
        tot = (slot(col_send, s) + slot(col_recv.at[0], s ^ 1)) + (slot(col_recv.at[1], s ^ 2) + slot(col_recv.at[2], s ^ 3))
        if s < 2:
            col_b[:, s * ROWS:(s + 1) * ROWS] = inv_count / tot
        else:
            for k in range(STEPS):
                start = X_BASE + (2 * k + s - 2) * CHUNK
                col_b[:, start:start + CHUNK] = inv_count / tot[:, k * CHUNK:(k + 1) * CHUNK]

    def d_img_chunk(r0):
        rows = pl.ds(r0, CHUNK)
        total = None
        for j in range(TXTS // 512):
            g = [exps[rows, c:c + 128] * (row_a[rows, :] + col_b[:, c:c + 128]) for c in range(j * 512, (j + 1) * 512, 128)]
            g = jnp.concatenate([v.astype(BF16) for v in g], axis=1)
            part = jnp.dot(g, txt[j * 512:(j + 1) * 512, :], preferred_element_type=F32)
            total = part if total is None else total + part
        return total

    def d_txt_chunk(c0):
        total = None
        for i in range(IMGS // 512):
            rows = slice(i * 512, (i + 1) * 512)
            g = []
            for q in range(CHUNK // 128):
                cols = pl.ds(c0 + q * 128, 128)
                g.append((exps[rows, cols] * (row_a[rows, :] + col_b[:, cols])).astype(BF16))
            g = jnp.concatenate(g, axis=1)
            part = lax.dot_general(g, img[rows, :], (((0,), (0,)), ((), ())), preferred_element_type=F32)
            total = part if total is None else total + part
        return total

    def chunk_of(k):
        return pl.ds(pl.multiple_of(k * CHUNK, CHUNK), CHUNK)

    def send_y(k):
        part = chunk_of(k)
        return to_y(d_img_send.at[part], d_img_recv.at[part], ry_send.at[k], ry_recv.at[k])

    def send_x(k):
        part = chunk_of(k)
        return to_row(d_txt_x.at[part], d_txt_recv.at[part], rx_send.at[k], rx_recv.at[k], across)

    def send_p(k, half, dst):
        n = half * STEPS + k
        return to_row(ring.at[lax.rem(k, 2)], dst.at[chunk_of(k)], rp_send.at[n], rp_recv.at[n], partner)

    send_s = [to_row(scal.at[0], scal.at[t + 1], sc_ssem.at[t], sc_rsem.at[t], peer) for t, peer in enumerate(peers)]

    def far_body(k, carry):
        part = chunk_of(k)
        x_cols = pl.multiple_of(X_BASE + 2 * k * CHUNK, CHUNK)
        @pl.when(k >= 2)
        def _():
            send_p(k - 2, 0, d_txt_x).wait_send()
        ring[lax.rem(k, 2)] = d_txt_chunk(x_cols + CHUNK)
        send_p(k, 0, d_txt_x).start()
        d_img_send[part, :] = d_img_chunk(pl.multiple_of(ROWS + k * CHUNK, CHUNK))
        send_y(k).start()
        mine = d_txt_chunk(x_cols)
        send_p(k, 0, d_txt_x).wait_recv()
        d_txt_x[part, :] += mine
        send_x(k).start()

        @pl.when(k == 0)
        def _():
            own_r = row_send[:, :ROWS] + row_recv[:, ROWS:]
            loss_part = jnp.sum(jnp.log(own_r) - jnp.log(col_b[:, :ROWS] / inv_count)) - 2.0 * scale * diag_sum
            dscale_part = scale * (jnp.sum(row_a[...] * row_m[...]) + jnp.sum(jnp.sum(col_m[...], axis=0, keepdims=True) * col_b[...])
                                   - 2.0 * inv_count * diag_sum)
            lane = lax.broadcasted_iota(jnp.int32, (8, 128), 1)
            scal[0] = jnp.where(lane == 0, loss_part * inv_count, dscale_part)
            for t in range(3):
                send_s[t].start()
        return carry
    lax.fori_loop(0, STEPS, far_body, 0)

    def fix_body(i, carry):
        part = pl.ds(pl.multiple_of(i * 128, 128), 128)
        on_diag = lax.broadcasted_iota(jnp.int32, (128, 128), 0) == lax.broadcasted_iota(jnp.int32, (128, 128), 1)
        term = (2.0 * inv_count) / (row_a[part, :] + col_b[:, part])
        exps[part, part] = exps[part, part] - jnp.where(on_diag, term, 0.0)
        return carry
    lax.fori_loop(0, ROWS // 128, fix_body, 0)

    def near_body(k, carry):
        part = chunk_of(k)
        @pl.when(k < 2)
        def _():
            send_p(k + 2, 0, d_txt_x).wait_send()
        @pl.when(k >= 2)
        def _():
            send_p(k - 2, 1, d_txt_p).wait_send()
        ring[lax.rem(k, 2)] = d_txt_chunk(pl.multiple_of(ROWS + k * CHUNK, CHUNK))
        send_p(k, 1, d_txt_p).start()
        d_img_own[part, :] = d_img_chunk(pl.multiple_of(k * CHUNK, CHUNK))
        mine = d_txt_chunk(pl.multiple_of(k * CHUNK, CHUNK))
        send_p(k, 1, d_txt_p).wait_recv()
        d_txt_p[part, :] += mine
        return carry
    lax.fori_loop(0, STEPS, near_body, 0)

    for t in range(3):
        send_s[t].wait_recv()
    scal_y[0] = (scal[0] + scal[1]) + (scal[2] + scal[3])
    swap_s = to_y(scal_y.at[0], scal_y.at[1], sc_ssem.at[3], sc_rsem.at[3])
    swap_s.start()

    outs = []
    for k in range(STEPS):
        part = pl.ds(k * CHUNK, CHUNK)
        slot_k = k % 2
        if k >= 2:
            outs[2 * k - 4].wait()
            outs[2 * k - 3].wait()
        send_y(k).wait_recv()
        out_stage[slot_k, 0] = (scale * (d_img_own[part, :] + d_img_recv[part, :])).astype(BF16)
        outs.append(pltpu.make_async_copy(out_stage.at[slot_k, 0], dimg_hbm.at[part], out_sem.at[2 * k]))
        outs[2 * k].start()
        send_x(k).wait_recv()
        out_stage[slot_k, 1] = (scale * (d_txt_p[part, :] + d_txt_recv[part, :])).astype(BF16)
        outs.append(pltpu.make_async_copy(out_stage.at[slot_k, 1], dtxt_hbm.at[part], out_sem.at[2 * k + 1]))
        outs[2 * k + 1].start()

    swap_s.wait_recv()
    total = scal_y[0] + scal_y[1]
    loss_ref[0, 0] = total[0, 0]
    dscale_ref[0, 0] = total[0, 1]

    for k in range(STEPS):
        gather_x[k].wait_send()
        gather_y[k].wait_send()
        relay[k].wait_send()
        send_y(k).wait_send()
        send_x(k).wait_send()
    gather_p.wait_send()
    swap_row.wait_send()
    for t in range(3):
        swap_col[t].wait_send()
        send_s[t].wait_send()
    swap_s.wait_send()
    for k in range(STEPS - 2, STEPS):
        send_p(k, 1, d_txt_p).wait_send()
    for k in range(2 * STEPS - 4, 2 * STEPS):
        outs[k].wait()


def solution(mesh):
    batch_spec = P(("row", "col"), None)
    n_dev = mesh.shape["row"] * mesh.shape["col"]
    inv_count = 1.0 / (2 * ROWS * n_dev)
    dma = pltpu.SemaphoreType.DMA

    def local_tile(img_loc, txt_loc, log_scale):
        any_spec = pl.BlockSpec(memory_space=pl.ANY)
        smem_spec = pl.BlockSpec(memory_space=pltpu.SMEM)
        loss, d_img, d_txt, d_scale = pl.pallas_call(
            functools.partial(kernel, inv_count),
            out_shape=(
                jax.ShapeDtypeStruct((1, 1), F32),
                jax.ShapeDtypeStruct((ROWS, DIM), BF16),
                jax.ShapeDtypeStruct((ROWS, DIM), BF16),
                jax.ShapeDtypeStruct((1, 1), F32),
            ),
            in_specs=[smem_spec, any_spec, any_spec],
            out_specs=(smem_spec, any_spec, any_spec, smem_spec),
            scratch_shapes=[
                pltpu.VMEM((IMGS, DIM), BF16),
                pltpu.VMEM((TXTS, DIM), BF16),
                pltpu.VMEM((IMGS, TXTS), F32),
                pltpu.VMEM((IMGS, 128), F32),
                pltpu.VMEM((IMGS, 128), F32),
                pltpu.VMEM((8, TXTS), F32),
                pltpu.VMEM((8, TXTS), F32),
                pltpu.VMEM((1, IMGS), F32),
                pltpu.VMEM((1, IMGS), F32),
                pltpu.VMEM((1, TXTS), F32),
                pltpu.VMEM((3, 1, TXTS), F32),
                pltpu.VMEM((1, TXTS), F32),
                pltpu.VMEM((ROWS, DIM), F32),
                pltpu.VMEM((ROWS, DIM), F32),
                pltpu.VMEM((ROWS, DIM), F32),
                pltpu.VMEM((2, CHUNK, DIM), F32),
                pltpu.VMEM((ROWS, DIM), F32),
                pltpu.VMEM((ROWS, DIM), F32),
                pltpu.VMEM((ROWS, DIM), F32),
                pltpu.VMEM((2, 2, CHUNK, DIM), BF16),
                pltpu.VMEM((4, 8, 128), F32),
                pltpu.VMEM((2, 8, 128), F32),
                dma((2,)),
                dma((STEPS,)), dma((STEPS,)),
                dma((STEPS,)), dma((STEPS,)),
                dma((2,)),
                dma((STEPS,)), dma((STEPS,)),
                dma((2,)),
                dma((3,)), dma((3,)),
                dma((STEPS,)), dma((STEPS,)),
                dma((2 * STEPS,)), dma((2 * STEPS,)),
                dma((STEPS,)), dma((STEPS,)),
                dma((4,)), dma((4,)),
                dma((2 * STEPS,)),
            ],
            compiler_params=pltpu.CompilerParams(
                collective_id=0, has_side_effects=True, vmem_limit_bytes=67043328,
            ),
            name="clip_loss",
        )(log_scale.reshape(1, 1), img_loc, txt_loc)
        return loss.reshape(()), d_img, d_txt, d_scale.reshape(())

    return jax.shard_map(local_tile, mesh=mesh, in_specs=(batch_spec, batch_spec, P()), out_specs=(P(), batch_spec, batch_spec, P()), check_vma=False)
```

```python
import functools
import math

import jax
import jax.numpy as jnp
from jax import lax
from jax.experimental import pallas as pl
from jax.experimental.pallas import tpu as pltpu
from jax.sharding import PartitionSpec as P

MESH = pl.DeviceIdType.MESH
VMEM_LIMIT = 61 * 1024 * 1024
F32 = jnp.float32
BF16 = jnp.bfloat16
ROWS = 1024
DIM = 512
CHUNK = 256
STEPS = ROWS // CHUNK
PIECE = 128
GATHER = (2, 2, 2, 1, 1)
G_START = tuple(sum(GATHER[:k]) for k in range(len(GATHER)))
G_STEPS = len(GATHER)
IMGS = 2 * ROWS
TXTS = 4 * ROWS
X_BASE = 2 * ROWS
LOG2E = math.log2(math.e)


def kernel(inv_count, scale_ref, img_hbm, txt_hbm, loss_ref, dimg_ref, dtxt_ref, dscale_ref,
           img, txt, far, txt_t, exps, row_e, row_m, col_e, col_m, row_send, row_recv, col_send, col_recv, col_b,
           d_img_send, d_img_recv, d_img_own, ring, d_txt_x, d_txt_p, d_txt_recv,
           scal, scal_y, load_sem, gy_send, gy_recv, gx_send, gx_recv, gp_sem, gf_send, gf_recv, row_sem, col_ssem, col_rsem,
           ry_send, ry_recv, rp_send, rp_recv, rx_send, rx_recv, sc_ssem, sc_rsem):
    row = lax.axis_index("row")
    col = lax.axis_index("col")
    core = lax.rem(row, 2)
    partner = row + 1 - 2 * core
    across = lax.rem(row + 2, 4)
    diagonal = across + 1 - 2 * core
    peers = (partner, across, diagonal)
    other_col = 1 - col

    def to_y(src, dst, ssem, rsem):
        return pltpu.make_async_remote_copy(src, dst, ssem, rsem, device_id={"row": row, "col": other_col}, device_id_type=MESH)

    def to_row(src, dst, ssem, rsem, peer):
        return pltpu.make_async_remote_copy(src, dst, ssem, rsem, device_id={"row": peer, "col": col}, device_id_type=MESH)

    load_img = pltpu.make_async_copy(img_hbm, img.at[pl.ds(0, ROWS)], load_sem.at[0])
    load_txt = pltpu.make_async_copy(txt_hbm, txt.at[0], load_sem.at[1])
    txt_pieces = txt.at[0].reshape(ROWS // PIECE, PIECE, DIM)
    load_img.start()
    load_txt.start()

    barrier = pltpu.get_barrier_semaphore()
    for peer in peers:
        pl.semaphore_signal(barrier, inc=1, device_id={"row": peer, "col": col}, device_id_type=MESH)
    pl.semaphore_signal(barrier, inc=1, device_id={"row": row, "col": other_col}, device_id_type=MESH)

    scale = jnp.max(jnp.exp(jnp.full((8, 128), scale_ref[0, 0], F32)))
    scale2 = scale * LOG2E
    row_e[...] = jnp.zeros_like(row_e)
    row_m[...] = jnp.zeros_like(row_m)
    col_e[...] = jnp.zeros_like(col_e)
    col_m[...] = jnp.zeros_like(col_m)

    load_img.wait()
    load_txt.wait()
    pl.semaphore_wait(barrier, 4)

    gather_y, gather_x, relay = [], [], []
    for k in range(G_STEPS):
        pieces = pl.ds(G_START[k], GATHER[k])
        part = pl.ds(G_START[k] * PIECE, GATHER[k] * PIECE)
        gather_x.append(to_row(txt_pieces.at[pieces], far.at[pieces, 0], gx_send.at[k], gx_recv.at[k], across))
        gather_y.append(to_y(img.at[part], img.at[pl.ds(ROWS + G_START[k] * PIECE, GATHER[k] * PIECE)], gy_send.at[k], gy_recv.at[k]))
        relay.append(to_row(far.at[pieces, 0], far.at[pieces, 1], gf_send.at[k], gf_recv.at[k], partner))
        gather_x[k].start()
        gather_y[k].start()
    gather_p = to_row(txt.at[0], txt.at[1], gp_sem.at[0], gp_sem.at[1], partner)
    gather_p.start()

    def logit_block(r0, nr, c0, nc, texts, on_rows):
        rows = pl.ds(r0, nr)
        cols = pl.ds(c0, nc)
        dots = lax.dot_general(img[rows, :], texts, (((1,), (1 if on_rows else 0,)), ((), ())), preferred_element_type=F32)
        e = jnp.exp2(dots * scale2)
        exps[rows, cols] = e
        m = e * dots
        for values, row_sum, col_sum in ((e, row_e, col_e), (m, row_m, col_m)):
            acc = values[:, 0:128]
            for q in range(1, nc // 128):
                acc = acc + values[:, q * 128:(q + 1) * 128]
            row_sum[rows, :] += acc
            col_sum[:, cols] += jnp.sum(values.reshape(nr // 8, 8, nc), axis=0)

    def own_by_held(slot):
        def body(i, carry):
            part = pl.ds(pl.multiple_of(i * 512, 512), 512)
            logit_block(0, ROWS, pl.multiple_of(slot * ROWS + i * 512, 512), 512, txt[slot, part, :], True)
            return carry
        lax.fori_loop(0, 2, body, 0)

    def turn_held(slot):
        def body(i, carry):
            part = pl.ds(pl.multiple_of(i * CHUNK, CHUNK), CHUNK)
            txt_t[:, pl.ds(pl.multiple_of(slot * ROWS + i * CHUNK, CHUNK), CHUNK)] = txt[slot, part, :].T
            return carry
        lax.fori_loop(0, STEPS, body, 0)

    own_by_held(0)
    turn_held(0)

    def diag_body(i, acc):
        part = pl.ds(pl.multiple_of(i * 128, 128), 128)
        prod = img[part, :].astype(F32) * txt[0, part, :].astype(F32)
        return acc + jnp.sum(prod.reshape(16, 8, DIM), axis=0)
    diag_sum = jnp.sum(lax.fori_loop(0, 8, diag_body, jnp.zeros((8, DIM), F32)))

    gather_p.wait_recv()
    own_by_held(1)
    turn_held(1)
    for k in range(G_STEPS):
        n_rows = GATHER[k] * PIECE
        done = G_START[k] * PIECE
        new_row = ROWS + done
        gather_x[k].wait_recv()
        relay[k].start()
        gather_y[k].wait_recv()
        def new_by_held(i, carry, new_row=new_row, n_rows=n_rows):
            c0 = pl.multiple_of(i * 1024, 1024)
            logit_block(new_row, n_rows, c0, 1024, txt_t[:, pl.ds(c0, 1024)], False)
            return carry
        n_held = X_BASE + 2 * done
        lax.fori_loop(0, n_held // 1024, new_by_held, 0)
        if n_held % 1024:
            c0 = n_held // 1024 * 1024
            logit_block(new_row, n_rows, c0, n_held - c0, txt_t[:, c0:n_held], False)
        relay[k].wait_recv()
        new_cols = 2 * n_rows
        logit_block(0, new_row + n_rows, n_held, new_cols, far[G_START[k]:G_START[k] + GATHER[k]].reshape(new_cols, DIM), True)
        if k + 1 < G_STEPS:
            for p in range(G_START[k], G_START[k] + GATHER[k]):
                c0 = X_BASE + 2 * p * PIECE
                txt_t[:, c0:c0 + 2 * PIECE] = far[p].reshape(2 * PIECE, DIM).T

    row_send[...] = jnp.sum(row_e[...].T, axis=0, keepdims=True)
    col_send[...] = jnp.sum(col_e[...], axis=0, keepdims=True)
    swap_row = to_y(row_send, row_recv, row_sem.at[0], row_sem.at[1])
    swap_row.start()
    swap_col = []
    for t, peer in enumerate(peers):
        swap_col.append(to_row(col_send, col_recv.at[t], col_ssem.at[t], col_rsem.at[t], peer))
        swap_col[t].start()
    swap_row.wait_recv()
    row_tot = row_send[...] + jnp.concatenate([row_recv[:, ROWS:], row_recv[:, :ROWS]], axis=1)
    row_a = row_e
    row_a[...] = jnp.broadcast_to(inv_count / row_tot, (128, IMGS)).T
    for t in range(3):
        swap_col[t].wait_recv()
    def slot(ref, s):
        if s < 2:
            return ref[:, s * ROWS:(s + 1) * ROWS]
        starts = [X_BASE + (2 * p + s - 2) * PIECE for p in range(ROWS // PIECE)]
        return jnp.concatenate([ref[:, c:c + PIECE] for c in starts], axis=1)
    for s in range(4):
        tot = (slot(col_send, s) + slot(col_recv.at[0], s ^ 1)) + (slot(col_recv.at[1], s ^ 2) + slot(col_recv.at[2], s ^ 3))
        inverse = inv_count / tot
        if s < 2:
            col_b[:, s * ROWS:(s + 1) * ROWS] = inverse
        else:
            for p in range(ROWS // PIECE):
                start = X_BASE + (2 * p + s - 2) * PIECE
                col_b[:, start:start + PIECE] = inverse[:, p * PIECE:(p + 1) * PIECE]

    def d_img_chunk(r0):
        rows = pl.ds(r0, CHUNK)
        total = None
        for j in range(TXTS // 512):
            g = [exps[rows, c:c + 128] * (row_a[rows, :] + col_b[:, c:c + 128]) for c in range(j * 512, (j + 1) * 512, 128)]
            g = jnp.concatenate([v.astype(BF16) for v in g], axis=1)
            texts = txt[j // 2, j % 2 * 512:(j % 2 + 1) * 512, :] if j < 4 else far[2 * j - 8:2 * j - 6].reshape(512, DIM)
            part = jnp.dot(g, texts, preferred_element_type=F32)
            total = part if total is None else total + part
        return total

    def d_txt_chunk(starts):
        total = None
        for i in range(IMGS // 512):
            rows = slice(i * 512, (i + 1) * 512)
            g = []
            for start in starts:
                cols = pl.ds(start, PIECE)
                g.append((exps[rows, cols] * (row_a[rows, :] + col_b[:, cols])).astype(BF16))
            g = jnp.concatenate(g, axis=1)
            part = lax.dot_general(g, img[rows, :], (((0,), (0,)), ((), ())), preferred_element_type=F32)
            total = part if total is None else total + part
        return total

    def chunk_of(k):
        return pl.ds(pl.multiple_of(k * CHUNK, CHUNK), CHUNK)

    def send_y(k):
        part = chunk_of(k)
        return to_y(d_img_send.at[part], d_img_recv.at[part], ry_send.at[k], ry_recv.at[k])

    def send_x(k):
        part = chunk_of(k)
        return to_row(d_txt_x.at[part], d_txt_recv.at[part], rx_send.at[k], rx_recv.at[k], across)

    def send_p(k, half, dst):
        n = half * STEPS + k
        return to_row(ring.at[lax.rem(k, 2)], dst.at[chunk_of(k)], rp_send.at[n], rp_recv.at[n], partner)

    send_s = [to_row(scal.at[0], scal.at[t + 1], sc_ssem.at[t], sc_rsem.at[t], peer) for t, peer in enumerate(peers)]

    def far_body(k, carry):
        part = chunk_of(k)
        x_cols = pl.multiple_of(X_BASE + 2 * k * CHUNK, CHUNK)
        same, other = (x_cols, x_cols + 2 * PIECE), (x_cols + PIECE, x_cols + 3 * PIECE)
        @pl.when(k >= 2)
        def _():
            send_p(k - 2, 0, d_txt_x).wait_send()
        ring[lax.rem(k, 2)] = d_txt_chunk(other)
        send_p(k, 0, d_txt_x).start()
        d_img_send[part, :] = d_img_chunk(pl.multiple_of(ROWS + k * CHUNK, CHUNK))
        send_y(k).start()
        mine = d_txt_chunk(same)
        send_p(k, 0, d_txt_x).wait_recv()
        d_txt_x[part, :] += mine
        send_x(k).start()

        @pl.when(k == 0)
        def _():
            own_r = row_send[:, :ROWS] + row_recv[:, ROWS:]
            loss_part = jnp.sum(jnp.log(own_r) - jnp.log(col_b[:, :ROWS] / inv_count)) - 2.0 * scale * diag_sum
            dscale_part = scale * (jnp.sum(row_a[...] * row_m[...]) + jnp.sum(jnp.sum(col_m[...], axis=0, keepdims=True) * col_b[...])
                                   - 2.0 * inv_count * diag_sum)
            lane = lax.broadcasted_iota(jnp.int32, (8, 128), 1)
            scal[0] = jnp.where(lane == 0, loss_part * inv_count, dscale_part)
            for t in range(3):
                send_s[t].start()
        return carry
    lax.fori_loop(0, STEPS, far_body, 0)

    def fix_body(i, carry):
        part = pl.ds(pl.multiple_of(i * 128, 128), 128)
        on_diag = lax.broadcasted_iota(jnp.int32, (128, 128), 0) == lax.broadcasted_iota(jnp.int32, (128, 128), 1)
        term = (2.0 * inv_count) / (row_a[part, :] + col_b[:, part])
        exps[part, part] = exps[part, part] - jnp.where(on_diag, term, 0.0)
        return carry
    lax.fori_loop(0, ROWS // 128, fix_body, 0)

    def near_body(k, carry):
        part = chunk_of(k)
        @pl.when(k < 2)
        def _():
            send_p(k + 2, 0, d_txt_x).wait_send()
        @pl.when(k >= 2)
        def _():
            send_p(k - 2, 1, d_txt_p).wait_send()
        first = pl.multiple_of(k * CHUNK, CHUNK)
        ring[lax.rem(k, 2)] = d_txt_chunk((ROWS + first, ROWS + first + PIECE))
        send_p(k, 1, d_txt_p).start()
        d_img_own[part, :] = d_img_chunk(first)
        mine = d_txt_chunk((first, first + PIECE))
        send_p(k, 1, d_txt_p).wait_recv()
        d_txt_p[part, :] += mine
        return carry
    lax.fori_loop(0, STEPS, near_body, 0)

    for t in range(3):
        send_s[t].wait_recv()
    scal_y[0] = (scal[0] + scal[1]) + (scal[2] + scal[3])
    swap_s = to_y(scal_y.at[0], scal_y.at[1], sc_ssem.at[3], sc_rsem.at[3])
    swap_s.start()

    def out_body(k, carry):
        part = chunk_of(k)
        send_y(k).wait_recv()
        dimg_ref[part, :] = (scale * (d_img_own[part, :] + d_img_recv[part, :])).astype(BF16)
        send_x(k).wait_recv()
        dtxt_ref[part, :] = (scale * (d_txt_p[part, :] + d_txt_recv[part, :])).astype(BF16)
        return carry
    lax.fori_loop(0, STEPS, out_body, 0)

    swap_s.wait_recv()
    total = scal_y[0] + scal_y[1]
    loss_ref[0, 0] = total[0, 0]
    dscale_ref[0, 0] = total[0, 1]

    for k in range(G_STEPS):
        gather_x[k].wait_send()
        gather_y[k].wait_send()
        relay[k].wait_send()
    for k in range(STEPS):
        send_y(k).wait_send()
        send_x(k).wait_send()
    gather_p.wait_send()
    swap_row.wait_send()
    for t in range(3):
        swap_col[t].wait_send()
        send_s[t].wait_send()
    swap_s.wait_send()
    for k in range(STEPS - 2, STEPS):
        send_p(k, 1, d_txt_p).wait_send()


def solution(mesh):
    batch_spec = P(("row", "col"), None)
    n_dev = mesh.shape["row"] * mesh.shape["col"]
    inv_count = 1.0 / (2 * ROWS * n_dev)
    dma = pltpu.SemaphoreType.DMA

    def local_tile(img_loc, txt_loc, log_scale):
        any_spec = pl.BlockSpec(memory_space=pl.ANY)
        vmem_spec = pl.BlockSpec(memory_space=pltpu.VMEM)
        smem_spec = pl.BlockSpec(memory_space=pltpu.SMEM)
        loss, d_img, d_txt, d_scale = pl.pallas_call(
            functools.partial(kernel, inv_count),
            out_shape=(
                jax.ShapeDtypeStruct((1, 1), F32),
                pltpu.VMEM((ROWS, DIM), BF16),
                pltpu.VMEM((ROWS, DIM), BF16),
                jax.ShapeDtypeStruct((1, 1), F32),
            ),
            in_specs=[smem_spec, any_spec, any_spec],
            out_specs=(smem_spec, vmem_spec, vmem_spec, smem_spec),
            scratch_shapes=[
                pltpu.VMEM((IMGS, DIM), BF16),
                pltpu.VMEM((2, ROWS, DIM), BF16),
                pltpu.VMEM((ROWS // PIECE, 2, PIECE, DIM), BF16),
                pltpu.VMEM((DIM, TXTS), BF16),
                pltpu.VMEM((IMGS, TXTS), F32),
                pltpu.VMEM((IMGS, 128), F32),
                pltpu.VMEM((IMGS, 128), F32),
                pltpu.VMEM((8, TXTS), F32),
                pltpu.VMEM((8, TXTS), F32),
                pltpu.VMEM((1, IMGS), F32),
                pltpu.VMEM((1, IMGS), F32),
                pltpu.VMEM((1, TXTS), F32),
                pltpu.VMEM((3, 1, TXTS), F32),
                pltpu.VMEM((1, TXTS), F32),
                pltpu.VMEM((ROWS, DIM), F32),
                pltpu.VMEM((ROWS, DIM), F32),
                pltpu.VMEM((ROWS, DIM), F32),
                pltpu.VMEM((2, CHUNK, DIM), F32),
                pltpu.VMEM((ROWS, DIM), F32),
                pltpu.VMEM((ROWS, DIM), F32),
                pltpu.VMEM((ROWS, DIM), F32),
                pltpu.VMEM((4, 8, 128), F32),
                pltpu.VMEM((2, 8, 128), F32),
                dma((2,)),
                dma((G_STEPS,)), dma((G_STEPS,)),
                dma((G_STEPS,)), dma((G_STEPS,)),
                dma((2,)),
                dma((G_STEPS,)), dma((G_STEPS,)),
                dma((2,)),
                dma((3,)), dma((3,)),
                dma((STEPS,)), dma((STEPS,)),
                dma((2 * STEPS,)), dma((2 * STEPS,)),
                dma((STEPS,)), dma((STEPS,)),
                dma((4,)), dma((4,)),
            ],
            compiler_params=pltpu.CompilerParams(
                collective_id=0, has_side_effects=True, vmem_limit_bytes=VMEM_LIMIT,
            ),
            name="clip_loss",
        )(log_scale.reshape(1, 1), img_loc, txt_loc)
        return loss.reshape(()), d_img, d_txt, d_scale.reshape(())

    return jax.shard_map(local_tile, mesh=mesh, in_specs=(batch_spec, batch_spec, P()), out_specs=(P(), batch_spec, batch_spec, P()), check_vma=False)
```

```python
import functools
import math

import jax
import jax.numpy as jnp
from jax import lax
from jax.experimental import pallas as pl
from jax.experimental.pallas import tpu as pltpu
from jax.sharding import PartitionSpec as P

MESH = pl.DeviceIdType.MESH
VMEM_LIMIT = 247 * 256 * 1024
F32 = jnp.float32
BF16 = jnp.bfloat16
ROWS = 1024
DIM = 512
CHUNK = 256
STEPS = ROWS // CHUNK
BULK = 2 * STEPS
PIECE = 128
GATHER = (2, 2, 2, 1, 1)
G_START = tuple(sum(GATHER[:k]) for k in range(len(GATHER)))
G_STEPS = len(GATHER)
IMGS = 2 * ROWS
TXTS = 4 * ROWS
X_BASE = 2 * ROWS
LOG2E = math.log2(math.e)


def kernel(inv_count, scale_ref, img_hbm, txt_hbm, loss_ref, dimg_ref, dtxt_ref, dscale_ref,
           img, txt, far, txt_t, img_p, new_txt, new_img, exps, row_e, row_m, col_e, col_m, row_send, row_recv, col_send, col_recv, col_b, row_l, all_a, all_b, new_b, txt_b,
           d_img_acc, d_txt_acc,
           scal, scal_y, load_sem, gy_send, gy_recv, gx_send, gx_recv, gp_sem, gf_send, gf_recv, row_sem, col_ssem, col_rsem,
           bx_send, bx_recv, by_send, by_recv, fx_send, fx_recv, fy_send, fy_recv, pn_send, pn_recv,
           a_ssem, a_rsem, b_sem, sc_ssem, sc_rsem):
    row = lax.axis_index("row")
    col = lax.axis_index("col")
    core = lax.rem(row, 2)
    partner = row + 1 - 2 * core
    across = lax.rem(row + 2, 4)
    diagonal = across + 1 - 2 * core
    peers = (partner, across, diagonal)
    other_col = 1 - col

    def to_y(src, dst, ssem, rsem):
        return pltpu.make_async_remote_copy(src, dst, ssem, rsem, device_id={"row": row, "col": other_col}, device_id_type=MESH)

    def to_row(src, dst, ssem, rsem, peer):
        return pltpu.make_async_remote_copy(src, dst, ssem, rsem, device_id={"row": peer, "col": col}, device_id_type=MESH)

    load_img = pltpu.make_async_copy(img_hbm, img.at[pl.ds(0, ROWS)], load_sem.at[0])
    load_txt = pltpu.make_async_copy(txt_hbm, txt.at[0], load_sem.at[1])
    txt_pieces = txt.at[0].reshape(ROWS // PIECE, PIECE, DIM)
    load_img.start()
    load_txt.start()

    barrier = pltpu.get_barrier_semaphore()
    for peer in peers:
        pl.semaphore_signal(barrier, inc=1, device_id={"row": peer, "col": col}, device_id_type=MESH)
    pl.semaphore_signal(barrier, inc=1, device_id={"row": row, "col": other_col}, device_id_type=MESH)

    scale = jnp.max(jnp.exp(jnp.full((8, 128), scale_ref[0, 0], F32)))
    scale2 = scale * LOG2E
    row_e[...] = jnp.zeros_like(row_e)
    row_m[...] = jnp.zeros_like(row_m)
    col_e[...] = jnp.zeros_like(col_e)
    col_m[...] = jnp.zeros_like(col_m)

    load_img.wait()
    load_txt.wait()
    with jax.named_scope("s1_pl_semaphore_wait_ba"):
        pl.semaphore_wait(barrier, 4)

    gather_y, gather_x, relay = [], [], []
    for k in range(G_STEPS):
        pieces = pl.ds(G_START[k], GATHER[k])
        part = pl.ds(G_START[k] * PIECE, GATHER[k] * PIECE)
        gather_x.append(to_row(txt_pieces.at[pieces], far.at[pieces, 0], gx_send.at[k], gx_recv.at[k], across))
        gather_y.append(to_y(img.at[part], img.at[pl.ds(ROWS + G_START[k] * PIECE, GATHER[k] * PIECE)], gy_send.at[k], gy_recv.at[k]))
        relay.append(to_row(far.at[pieces, 0], far.at[pieces, 1], gf_send.at[k], gf_recv.at[k], partner))
        gather_x[k].start()
        gather_y[k].start()
    gather_p = to_row(txt.at[0], txt.at[1], gp_sem.at[0], gp_sem.at[1], partner)
    gather_p.start()
    gather_i = to_row(img.at[pl.ds(0, ROWS)], img_p.at[pl.ds(0, ROWS)], gp_sem.at[2], gp_sem.at[3], partner)
    gather_i.start()
    relay_n = []
    for k in range(G_STEPS):
        part = pl.ds(ROWS + G_START[k] * PIECE, GATHER[k] * PIECE)
        relay_n.append(to_row(img.at[part], img_p.at[part], pn_send.at[k], pn_recv.at[k], partner))

    img_pieces = img.reshape(IMGS // PIECE, PIECE, DIM)
    new_img_pieces = new_img.reshape(2, IMGS // PIECE, PIECE, DIM)
    new_txt_pieces = new_txt.reshape(2, IMGS // PIECE, PIECE, DIM)
    bulk_x, bulk_y = [], []
    for k in range(BULK):
        two = pl.ds(2 * k, 2)
        bulk_x.append(to_row(img_pieces.at[two], new_img_pieces.at[0, two], bx_send.at[k], bx_recv.at[k], across))
        source = txt_pieces.at[two] if k < BULK // 2 else far.at[pl.ds(2 * k - BULK, 2), 0]
        bulk_y.append(to_y(source, new_txt_pieces.at[0, two], by_send.at[k], by_recv.at[k]))
    bulk_x[0].start()
    bulk_y[0].start()

    def logit_block(r0, nr, c0, nc, texts, on_rows):
        rows = pl.ds(r0, nr)
        cols = pl.ds(c0, nc)
        dots = lax.dot_general(img[rows, :], texts, (((1,), (1 if on_rows else 0,)), ((), ())), preferred_element_type=F32)
        e = jnp.exp2(dots * scale2)
        exps[rows, cols] = e
        m = e * dots
        for values, row_sum, col_sum in ((e, row_e, col_e), (m, row_m, col_m)):
            acc = values[:, 0:128]
            for q in range(1, nc // 128):
                acc = acc + values[:, q * 128:(q + 1) * 128]
            row_sum[rows, :] += acc
            col_sum[:, cols] += jnp.sum(values.reshape(nr // 8, 8, nc), axis=0)

    def own_by_held(slot):
        def body(i, carry):
            part = pl.ds(pl.multiple_of(i * 512, 512), 512)
            logit_block(0, ROWS, pl.multiple_of(slot * ROWS + i * 512, 512), 512, txt[slot, part, :], True)
            return carry
        lax.fori_loop(0, 2, body, 0)

    def turn_held(slot):
        def body(i, carry):
            part = pl.ds(pl.multiple_of(i * CHUNK, CHUNK), CHUNK)
            txt_t[:, pl.ds(pl.multiple_of(slot * ROWS + i * CHUNK, CHUNK), CHUNK)] = txt[slot, part, :].T
            return carry
        lax.fori_loop(0, STEPS, body, 0)

    with jax.named_scope("s2_own_by_held_0_"):
        own_by_held(0)
    with jax.named_scope("s3_turn_held_0_"):
        turn_held(0)

    def diag_body(i, acc):
        part = pl.ds(pl.multiple_of(i * 128, 128), 128)
        prod = img[part, :].astype(F32) * txt[0, part, :].astype(F32)
        return acc + jnp.sum(prod.reshape(16, 8, DIM), axis=0)
    diag_sum = jnp.sum(lax.fori_loop(0, 8, diag_body, jnp.zeros((8, DIM), F32)))

    with jax.named_scope("s4_gather_p_wait_recv_"):
        gather_p.wait_recv()
    with jax.named_scope("s5_own_by_held_1_"):
        own_by_held(1)
    with jax.named_scope("s6_turn_held_1_"):
        turn_held(1)
    for k in range(G_STEPS):
        n_rows = GATHER[k] * PIECE
        done = G_START[k] * PIECE
        new_row = ROWS + done
        with jax.named_scope("s7_gather_x_k_wait_recv"):
            gather_x[k].wait_recv()
        relay[k].start()
        with jax.named_scope("s8_gather_y_k_wait_recv"):
            gather_y[k].wait_recv()
        relay_n[k].start()
        def new_by_held(i, carry, new_row=new_row, n_rows=n_rows):
            c0 = pl.multiple_of(i * 1024, 1024)
            logit_block(new_row, n_rows, c0, 1024, txt_t[:, pl.ds(c0, 1024)], False)
            return carry
        n_held = X_BASE + 2 * done
        with jax.named_scope("s9_lax_fori_loop_0_n_he"):
            lax.fori_loop(0, n_held // 1024, new_by_held, 0)
        if n_held % 1024:
            c0 = n_held // 1024 * 1024
            logit_block(new_row, n_rows, c0, n_held - c0, txt_t[:, c0:n_held], False)
        with jax.named_scope("s10_relay_k_wait_recv_"):
            relay[k].wait_recv()
        new_cols = 2 * n_rows
        with jax.named_scope("s11_logit_block_0_new_ro"):
            logit_block(0, new_row + n_rows, n_held, new_cols, far[G_START[k]:G_START[k] + GATHER[k]].reshape(new_cols, DIM), True)
        if k + 1 < G_STEPS:
            for p in range(G_START[k], G_START[k] + GATHER[k]):
                c0 = X_BASE + 2 * p * PIECE
                txt_t[:, c0:c0 + 2 * PIECE] = far[p].reshape(2 * PIECE, DIM).T

    with jax.named_scope("s12_row_send_jnp_sum_row"):
        row_send[...] = jnp.sum(row_e[...].T, axis=0, keepdims=True)
    col_send[...] = jnp.sum(col_e[...], axis=0, keepdims=True)
    swap_row = to_y(row_send, row_recv, row_sem.at[0], row_sem.at[1])
    swap_row.start()
    swap_col = []
    for t, peer in enumerate(peers):
        swap_col.append(to_row(col_send, col_recv.at[t], col_ssem.at[t], col_rsem.at[t], peer))
        swap_col[t].start()
    bulk_x[1].start()
    bulk_y[1].start()
    with jax.named_scope("s13_swap_row_wait_recv_"):
        swap_row.wait_recv()
    row_tot = row_send[...] + jnp.concatenate([row_recv[:, ROWS:], row_recv[:, :ROWS]], axis=1)
    row_a = row_e
    row_l[...] = inv_count / row_tot
    swap_a = []
    for t, peer in enumerate(peers):
        swap_a.append(to_row(row_l, all_a.at[t], a_ssem.at[t], a_rsem.at[t], peer))
        swap_a[t].start()
    with jax.named_scope("s14_row_a_jnp_broadcast_"):
        row_a[...] = jnp.broadcast_to(row_l[...], (128, IMGS)).T
    for t in range(3):
        with jax.named_scope("s15_swap_col_t_wait_recv"):
            swap_col[t].wait_recv()
    def slot(ref, s):
        if s < 2:
            return ref[:, s * ROWS:(s + 1) * ROWS]
        starts = [X_BASE + (2 * p + s - 2) * PIECE for p in range(ROWS // PIECE)]
        return jnp.concatenate([ref[:, c:c + PIECE] for c in starts], axis=1)
    for s in range(4):
        tot = (slot(col_send, s) + slot(col_recv.at[0], s ^ 1)) + (slot(col_recv.at[1], s ^ 2) + slot(col_recv.at[2], s ^ 3))
        inverse = inv_count / tot
        if s < 2:
            col_b[:, s * ROWS:(s + 1) * ROWS] = inverse
        else:
            for p in range(ROWS // PIECE):
                start = X_BASE + (2 * p + s - 2) * PIECE
                col_b[:, start:start + PIECE] = inverse[:, p * PIECE:(p + 1) * PIECE]

    def d_img_chunk(r0):
        rows = pl.ds(r0, CHUNK)
        total = None
        for j in range(TXTS // 512):
            g = [exps[rows, c:c + 128] * (row_a[rows, :] + col_b[:, c:c + 128]) for c in range(j * 512, (j + 1) * 512, 128)]
            g = jnp.concatenate([v.astype(BF16) for v in g], axis=1)
            texts = txt[j // 2, j % 2 * 512:(j % 2 + 1) * 512, :] if j < 4 else far[2 * j - 8:2 * j - 6].reshape(512, DIM)
            part = jnp.dot(g, texts, preferred_element_type=F32)
            total = part if total is None else total + part
        return total

    def d_txt_chunk(starts):
        total = None
        for i in range(IMGS // 512):
            rows = slice(i * 512, (i + 1) * 512)
            g = []
            for start in starts:
                cols = pl.ds(start, PIECE)
                g.append((exps[rows, cols] * (row_a[rows, :] + col_b[:, cols])).astype(BF16))
            g = jnp.concatenate(g, axis=1)
            part = lax.dot_general(g, img[rows, :], (((0,), (0,)), ((), ())), preferred_element_type=F32)
            total = part if total is None else total + part
        return total

    swap_b = to_y(col_b, all_b, b_sem.at[0], b_sem.at[1])
    swap_b.start()
    own_r = row_send[:, :ROWS] + row_recv[:, ROWS:]
    loss_part = jnp.sum(jnp.log(own_r) - jnp.log(col_b[:, :ROWS] / inv_count)) - 2.0 * scale * diag_sum
    dscale_part = scale * (jnp.sum(row_a[...] * row_m[...]) + jnp.sum(jnp.sum(col_m[...], axis=0, keepdims=True) * col_b[...])
                           - 2.0 * inv_count * diag_sum)
    lane = lax.broadcasted_iota(jnp.int32, (8, 128), 1)
    scal[0] = jnp.where(lane == 0, loss_part * inv_count, dscale_part)
    send_s = [to_row(scal.at[0], scal.at[t + 1], sc_ssem.at[t], sc_rsem.at[t], peer) for t, peer in enumerate(peers)]
    for t in range(3):
        send_s[t].start()
    for k in range(2, BULK):
        bulk_x[k].start()
        bulk_y[k].start()

    def fix_body(i, carry):
        part = pl.ds(pl.multiple_of(i * 128, 128), 128)
        on_diag = lax.broadcasted_iota(jnp.int32, (128, 128), 0) == lax.broadcasted_iota(jnp.int32, (128, 128), 1)
        term = (2.0 * inv_count) / (row_a[part, :] + col_b[:, part])
        exps[part, part] = exps[part, part] - jnp.where(on_diag, term, 0.0)
        return carry
    with jax.named_scope("s16_lax_fori_loop_0_ROWS"):
        lax.fori_loop(0, ROWS // 128, fix_body, 0)
    txt_b[...] = jnp.broadcast_to(col_b[:, :ROWS], (128, ROWS)).T

    def tile_body(k, carry):
        first = pl.multiple_of(k * CHUNK, CHUNK)
        part = pl.ds(first, CHUNK)
        with jax.named_scope("s17_d_img_acc_part_d_img"):
            d_img_acc[part, :] = d_img_chunk(first)
        with jax.named_scope("s18_d_txt_acc_part_d_txt"):
            d_txt_acc[part, :] = d_txt_chunk((first, first + PIECE))
        return carry
    with jax.named_scope("s19_lax_fori_loop_0_STEP"):
        lax.fori_loop(0, STEPS, tile_body, 0)

    for t in range(3):
        with jax.named_scope("s20_swap_a_t_wait_recv_"):
            swap_a[t].wait_recv()
        with jax.named_scope("s21_send_s_t_wait_recv_"):
            send_s[t].wait_recv()
    with jax.named_scope("s22_swap_b_wait_recv_"):
        swap_b.wait_recv()
    for s in range(2):
        new_b[s, :, :ROWS] = slot(all_b, s)
        new_b[s, :, ROWS:] = slot(all_b, s + 2)
    scal_y[0] = (scal[0] + scal[1]) + (scal[2] + scal[3])
    swap_s = to_y(scal_y.at[0], scal_y.at[1], sc_ssem.at[3], sc_rsem.at[3])
    swap_s.start()

    def outside(own, own_factor, others, factor, total):
        dots = lax.dot_general(own, others, (((1,), (1,)), ((), ())), preferred_element_type=F32)
        e = jnp.exp2(dots * scale2)
        g = [(e[:, c:c + 128] * (own_factor + factor[:, c:c + 128])).astype(BF16) for c in range(0, CHUNK, 128)]
        total[...] += jnp.dot(jnp.concatenate(g, axis=1), others, preferred_element_type=F32)

    def more_img(others, factor):
        outside(img[0:ROWS, :], row_a[0:ROWS, :], others, factor, d_img_acc)

    def more_txt(others, factor):
        outside(txt[0], txt_b[...], others, factor, d_txt_acc)

    with jax.named_scope("s23_gather_i_wait_recv_"):
        gather_i.wait_recv()
    for k in range(G_STEPS):
        with jax.named_scope("s24_relay_n_k_wait_recv_"):
            relay_n[k].wait_recv()

    def partner_body(k, carry):
        part = pl.ds(pl.multiple_of(k * CHUNK, CHUNK), CHUNK)
        more_txt(img_p[part, :], all_a[0, :, part])
        return carry
    with jax.named_scope("s25_lax_fori_loop_0_IMGS"):
        lax.fori_loop(0, IMGS // CHUNK, partner_body, 0)

    def bulk_of(k):
        two = pl.ds(2 * k, 2)
        x = to_row(new_img_pieces.at[0, two], new_img_pieces.at[0, two], bx_send.at[k], bx_recv.at[k], across)
        y = to_y(new_txt_pieces.at[0, two], new_txt_pieces.at[0, two], by_send.at[k], by_recv.at[k])
        return x, y

    def relay_of(k):
        part = pl.ds(pl.multiple_of(k * CHUNK, CHUNK), CHUNK)
        x = to_row(new_img.at[0, part], new_img.at[1, part], fx_send.at[k], fx_recv.at[k], partner)
        y = to_row(new_txt.at[0, part], new_txt.at[1, part], fy_send.at[k], fy_recv.at[k], partner)
        return x, y

    def bulk_body(k, carry):
        part = pl.ds(pl.multiple_of(k * CHUNK, CHUNK), CHUNK)
        x, y = bulk_of(k)
        rx, ry = relay_of(k)
        with jax.named_scope("s26_x_wait_recv_"):
            x.wait_recv()
        rx.start()
        with jax.named_scope("s27_y_wait_recv_"):
            y.wait_recv()
        ry.start()
        with jax.named_scope("s28_more_txt_new_img_0_p"):
            more_txt(new_img[0, part, :], all_a[1, :, part])
        with jax.named_scope("s29_more_img_new_txt_0_p"):
            more_img(new_txt[0, part, :], new_b[0, :, part])
        with jax.named_scope("s30_rx_wait_recv_"):
            rx.wait_recv()
        with jax.named_scope("s31_more_txt_new_img_1_p"):
            more_txt(new_img[1, part, :], all_a[2, :, part])
        with jax.named_scope("s32_ry_wait_recv_"):
            ry.wait_recv()
        with jax.named_scope("s33_more_img_new_txt_1_p"):
            more_img(new_txt[1, part, :], new_b[1, :, part])
        return carry
    lax.fori_loop(0, BULK, bulk_body, 0)

    with jax.named_scope("s34_dimg_ref_scale_d_img"):
        dimg_ref[...] = (scale * d_img_acc[...]).astype(BF16)
    dtxt_ref[...] = (scale * d_txt_acc[...]).astype(BF16)

    with jax.named_scope("s35_swap_s_wait_recv_"):
        swap_s.wait_recv()
    total = scal_y[0] + scal_y[1]
    loss_ref[0, 0] = total[0, 0]
    dscale_ref[0, 0] = total[0, 1]

    for k in range(G_STEPS):
        gather_x[k].wait_send()
        gather_y[k].wait_send()
        relay[k].wait_send()
        relay_n[k].wait_send()
    for k in range(BULK):
        bulk_x[k].wait_send()
        bulk_y[k].wait_send()
        for copy in relay_of(k):
            copy.wait_send()
    gather_p.wait_send()
    gather_i.wait_send()
    swap_b.wait_send()
    swap_row.wait_send()
    for t in range(3):
        swap_col[t].wait_send()
        send_s[t].wait_send()
        swap_a[t].wait_send()
    swap_s.wait_send()


def solution(mesh):
    batch_spec = P(("row", "col"), None)
    n_dev = mesh.shape["row"] * mesh.shape["col"]
    inv_count = 1.0 / (2 * ROWS * n_dev)
    dma = pltpu.SemaphoreType.DMA

    def local_tile(img_loc, txt_loc, log_scale):
        any_spec = pl.BlockSpec(memory_space=pl.ANY)
        vmem_spec = pl.BlockSpec(memory_space=pltpu.VMEM)
        smem_spec = pl.BlockSpec(memory_space=pltpu.SMEM)
        loss, d_img, d_txt, d_scale = pl.pallas_call(
            functools.partial(kernel, inv_count),
            out_shape=(
                jax.ShapeDtypeStruct((1, 1), F32),
                pltpu.VMEM((ROWS, DIM), BF16),
                pltpu.VMEM((ROWS, DIM), BF16),
                jax.ShapeDtypeStruct((1, 1), F32),
            ),
            in_specs=[smem_spec, any_spec, any_spec],
            out_specs=(smem_spec, vmem_spec, vmem_spec, smem_spec),
            scratch_shapes=[
                pltpu.VMEM((IMGS, DIM), BF16),
                pltpu.VMEM((2, ROWS, DIM), BF16),
                pltpu.VMEM((ROWS // PIECE, 2, PIECE, DIM), BF16),
                pltpu.VMEM((DIM, TXTS), BF16),
                pltpu.VMEM((IMGS, DIM), BF16),
                pltpu.VMEM((2, IMGS, DIM), BF16),
                pltpu.VMEM((2, IMGS, DIM), BF16),
                pltpu.VMEM((IMGS, TXTS), F32),
                pltpu.VMEM((IMGS, 128), F32),
                pltpu.VMEM((IMGS, 128), F32),
                pltpu.VMEM((8, TXTS), F32),
                pltpu.VMEM((8, TXTS), F32),
                pltpu.VMEM((1, IMGS), F32),
                pltpu.VMEM((1, IMGS), F32),
                pltpu.VMEM((1, TXTS), F32),
                pltpu.VMEM((3, 1, TXTS), F32),
                pltpu.VMEM((1, TXTS), F32),
                pltpu.VMEM((1, IMGS), F32),
                pltpu.VMEM((3, 1, IMGS), F32),
                pltpu.VMEM((1, TXTS), F32),
                pltpu.VMEM((2, 1, IMGS), F32),
                pltpu.VMEM((ROWS, 128), F32),
                pltpu.VMEM((ROWS, DIM), F32),
                pltpu.VMEM((ROWS, DIM), F32),
                pltpu.VMEM((4, 8, 128), F32),
                pltpu.VMEM((2, 8, 128), F32),
                dma((2,)),
                dma((G_STEPS,)), dma((G_STEPS,)),
                dma((G_STEPS,)), dma((G_STEPS,)),
                dma((4,)),
                dma((G_STEPS,)), dma((G_STEPS,)),
                dma((2,)),
                dma((3,)), dma((3,)),
                dma((BULK,)), dma((BULK,)), dma((BULK,)), dma((BULK,)),
                dma((BULK,)), dma((BULK,)), dma((BULK,)), dma((BULK,)),
                dma((G_STEPS,)), dma((G_STEPS,)),
                dma((3,)), dma((3,)), dma((2,)),
                dma((4,)), dma((4,)),
            ],
            compiler_params=pltpu.CompilerParams(
                collective_id=0, has_side_effects=True, vmem_limit_bytes=VMEM_LIMIT,
            ),
            name="clip_loss",
        )(log_scale.reshape(1, 1), img_loc, txt_loc)
        return loss.reshape(()), d_img, d_txt, d_scale.reshape(())

    return jax.shard_map(local_tile, mesh=mesh, in_specs=(batch_spec, batch_spec, P()), out_specs=(P(), batch_spec, batch_spec, P()), check_vma=False)
```

```python
import functools
import math

import jax
import jax.numpy as jnp
from jax import lax
from jax.experimental import pallas as pl
from jax.experimental.pallas import tpu as pltpu
from jax.sharding import PartitionSpec as P

MESH = pl.DeviceIdType.MESH
VMEM_LIMIT = 247 * 256 * 1024
F32 = jnp.float32
BF16 = jnp.bfloat16
ROWS = 1024
DIM = 512
CHUNK = 256
STEPS = ROWS // CHUNK
BULK = 2 * STEPS + 1
WHOLE = BULK - 2
PIECE = 128
GATHER = (2, 2, 2, 1, 1)
G_START = tuple(sum(GATHER[:k]) for k in range(len(GATHER)))
G_STEPS = len(GATHER)
IMGS = 2 * ROWS
TXTS = 4 * ROWS
X_BASE = 2 * ROWS
LOG2E = math.log2(math.e)


def kernel(inv_count, scale_ref, img_hbm, txt_hbm, loss_ref, dimg_ref, dtxt_ref, dscale_ref,
           img, txt, far, txt_t, img_p, new_txt, new_img, exps, row_e, row_m, col_e, col_m, row_send, row_recv, col_send, col_recv, col_b, row_l, all_a, all_b, new_a, new_b, txt_b,
           scal, scal_y, load_sem, gy_send, gy_recv, gx_send, gx_recv, gp_sem, gf_send, gf_recv, row_sem, col_ssem, col_rsem,
           bx_send, bx_recv, by_send, by_recv, fx_send, fx_recv, fy_send, fy_recv, pn_send, pn_recv,
           a_ssem, a_rsem, b_sem, sc_ssem, sc_rsem):
    row = lax.axis_index("row")
    col = lax.axis_index("col")
    core = lax.rem(row, 2)
    partner = row + 1 - 2 * core
    across = lax.rem(row + 2, 4)
    diagonal = across + 1 - 2 * core
    peers = (partner, across, diagonal)
    other_col = 1 - col

    def to_y(src, dst, ssem, rsem):
        return pltpu.make_async_remote_copy(src, dst, ssem, rsem, device_id={"row": row, "col": other_col}, device_id_type=MESH)

    def to_row(src, dst, ssem, rsem, peer):
        return pltpu.make_async_remote_copy(src, dst, ssem, rsem, device_id={"row": peer, "col": col}, device_id_type=MESH)

    load_img = pltpu.make_async_copy(img_hbm, img.at[pl.ds(0, ROWS)], load_sem.at[0])
    load_txt = pltpu.make_async_copy(txt_hbm, txt.at[0], load_sem.at[1])
    txt_pieces = txt.at[0].reshape(ROWS // PIECE, PIECE, DIM)
    load_img.start()
    load_txt.start()

    barrier = pltpu.get_barrier_semaphore()
    for peer in peers:
        pl.semaphore_signal(barrier, inc=1, device_id={"row": peer, "col": col}, device_id_type=MESH)
    pl.semaphore_signal(barrier, inc=1, device_id={"row": row, "col": other_col}, device_id_type=MESH)

    scale = jnp.max(jnp.exp(jnp.full((8, 128), scale_ref[0, 0], F32)))
    scale2 = scale * LOG2E
    row_e[...] = jnp.zeros_like(row_e)
    row_m[...] = jnp.zeros_like(row_m)
    col_e[...] = jnp.zeros_like(col_e)
    col_m[...] = jnp.zeros_like(col_m)

    load_img.wait()
    load_txt.wait()
    with jax.named_scope("s1_pl_semaphore_wait_ba"):
        pl.semaphore_wait(barrier, 4)

    gather_y, gather_x, relay = [], [], []
    for k in range(G_STEPS):
        pieces = pl.ds(G_START[k], GATHER[k])
        part = pl.ds(G_START[k] * PIECE, GATHER[k] * PIECE)
        gather_x.append(to_row(txt_pieces.at[pieces], far.at[pieces, 0], gx_send.at[k], gx_recv.at[k], across))
        gather_y.append(to_y(img.at[part], img.at[pl.ds(ROWS + G_START[k] * PIECE, GATHER[k] * PIECE)], gy_send.at[k], gy_recv.at[k]))
        relay.append(to_row(far.at[pieces, 0], far.at[pieces, 1], gf_send.at[k], gf_recv.at[k], partner))
        gather_x[k].start()
        gather_y[k].start()
    gather_p = to_row(txt.at[0], txt.at[1], gp_sem.at[0], gp_sem.at[1], partner)
    gather_p.start()
    gather_i = to_row(img.at[pl.ds(0, ROWS)], img_p.at[pl.ds(0, ROWS)], gp_sem.at[2], gp_sem.at[3], partner)
    gather_i.start()
    relay_n = []
    for k in range(G_STEPS):
        part = pl.ds(ROWS + G_START[k] * PIECE, GATHER[k] * PIECE)
        relay_n.append(to_row(img.at[part], img_p.at[part], pn_send.at[k], pn_recv.at[k], partner))

    img_pieces = img.reshape(IMGS // PIECE, PIECE, DIM)
    new_img_pieces = new_img.reshape(TXTS // PIECE, PIECE, DIM)
    new_txt_pieces = new_txt.reshape(TXTS // PIECE, PIECE, DIM)

    def bulk_span(k):
        return (2 * k, 4 * k, 2) if k < WHOLE else (WHOLE + k, 2 * (WHOLE + k), 1)

    bulk_x, bulk_y = [], []
    for k in range(BULK):
        src, dst, size = bulk_span(k)
        land = pl.ds(dst, size)
        bulk_x.append(to_row(img_pieces.at[pl.ds(src, size)], new_img_pieces.at[land], bx_send.at[k], bx_recv.at[k], across))
        half = ROWS // PIECE
        source = txt_pieces.at[pl.ds(src, size)] if src < half else far.at[pl.ds(src - half, size), 0]
        bulk_y.append(to_y(source, new_txt_pieces.at[land], by_send.at[k], by_recv.at[k]))
    bulk_x[0].start()
    bulk_y[0].start()

    def logit_block(r0, nr, c0, nc, texts, on_rows, kept):
        rows = pl.ds(r0, nr)
        cols = pl.ds(c0, nc)
        dots = lax.dot_general(img[rows, :], texts, (((1,), (1 if on_rows else 0,)), ((), ())), preferred_element_type=F32)
        e = jnp.exp2(dots * scale2)
        if kept:
            exps[pl.ds(r0, kept), cols] = e[:kept]
        m = e * dots
        for values, row_sum, col_sum in ((e, row_e, col_e), (m, row_m, col_m)):
            acc = values[:, 0:128]
            for q in range(1, nc // 128):
                acc = acc + values[:, q * 128:(q + 1) * 128]
            row_sum[rows, :] += acc
            col_sum[:, cols] += jnp.sum(values.reshape(nr // 8, 8, nc), axis=0)

    def own_by_held(slot):
        def body(i, carry):
            part = pl.ds(pl.multiple_of(i * 512, 512), 512)
            logit_block(0, ROWS, pl.multiple_of(slot * ROWS + i * 512, 512), 512, txt[slot, part, :], True, ROWS)
            return carry
        lax.fori_loop(0, 2, body, 0)

    def turn_held(slot):
        def body(i, carry):
            part = pl.ds(pl.multiple_of(i * CHUNK, CHUNK), CHUNK)
            txt_t[:, pl.ds(pl.multiple_of(slot * ROWS + i * CHUNK, CHUNK), CHUNK)] = txt[slot, part, :].T
            return carry
        lax.fori_loop(0, STEPS, body, 0)

    def partner_exps(c0, n):
        dots = lax.dot_general(txt[0], img_p[pl.ds(c0, n), :], (((1,), (1,)), ((), ())), preferred_element_type=F32)
        exps[ROWS:, pl.ds(ROWS + c0, n)] = jnp.exp2(dots * scale2)

    with jax.named_scope("s2_own_by_held_0_"):
        own_by_held(0)
    with jax.named_scope("s3_turn_held_0_"):
        turn_held(0)

    def diag_body(i, acc):
        part = pl.ds(pl.multiple_of(i * 128, 128), 128)
        prod = img[part, :].astype(F32) * txt[0, part, :].astype(F32)
        return acc + jnp.sum(prod.reshape(16, 8, DIM), axis=0)
    diag_sum = jnp.sum(lax.fori_loop(0, 8, diag_body, jnp.zeros((8, DIM), F32)))

    with jax.named_scope("s4_gather_p_wait_recv_"):
        gather_p.wait_recv()
    with jax.named_scope("s5_own_by_held_1_"):
        own_by_held(1)
    with jax.named_scope("s6_turn_held_1_"):
        turn_held(1)
    with jax.named_scope("s7_gather_i_wait_recv_"):
        gather_i.wait_recv()
    def partner_own(i, carry):
        with jax.named_scope("s8_partner_exps_pl_mult"):
            partner_exps(pl.multiple_of(i * 512, 512), 512)
        return carry
    with jax.named_scope("s9_lax_fori_loop_0_2_pa"):
        lax.fori_loop(0, 2, partner_own, 0)
    for k in range(G_STEPS):
        n_rows = GATHER[k] * PIECE
        done = G_START[k] * PIECE
        new_row = ROWS + done
        with jax.named_scope("s10_gather_x_k_wait_recv"):
            gather_x[k].wait_recv()
        relay[k].start()
        with jax.named_scope("s11_gather_y_k_wait_recv"):
            gather_y[k].wait_recv()
        relay_n[k].start()
        def new_by_held(i, carry, new_row=new_row, n_rows=n_rows):
            c0 = pl.multiple_of(i * 1024, 1024)
            logit_block(new_row, n_rows, c0, 1024, txt_t[:, pl.ds(c0, 1024)], False, 0)
            return carry
        n_held = X_BASE + 2 * done
        logit_block(new_row, n_rows, 0, ROWS, txt_t[:, :ROWS], False, n_rows)
        with jax.named_scope("s12_lax_fori_loop_1_n_he"):
            lax.fori_loop(1, n_held // 1024, new_by_held, 0)
        if n_held % 1024:
            c0 = n_held // 1024 * 1024
            logit_block(new_row, n_rows, c0, n_held - c0, txt_t[:, c0:n_held], False, 0)
        with jax.named_scope("s13_relay_k_wait_recv_"):
            relay[k].wait_recv()
        new_cols = 2 * n_rows
        with jax.named_scope("s14_logit_block_0_new_ro"):
            logit_block(0, new_row + n_rows, n_held, new_cols, far[G_START[k]:G_START[k] + GATHER[k]].reshape(new_cols, DIM), True, ROWS)
        if k + 1 < G_STEPS:
            for p in range(G_START[k], G_START[k] + GATHER[k]):
                c0 = X_BASE + 2 * p * PIECE
                txt_t[:, c0:c0 + 2 * PIECE] = far[p].reshape(2 * PIECE, DIM).T
        if k < 3:
            relay_n[k].wait_recv()
            partner_exps(ROWS + k * CHUNK, CHUNK)

    with jax.named_scope("s15_row_send_jnp_sum_row"):
        row_send[...] = jnp.sum(row_e[...].T, axis=0, keepdims=True)
    col_send[...] = jnp.sum(col_e[...], axis=0, keepdims=True)
    swap_row = to_y(row_send, row_recv, row_sem.at[0], row_sem.at[1])
    swap_row.start()
    swap_col = []
    for t, peer in enumerate(peers):
        swap_col.append(to_row(col_send, col_recv.at[t], col_ssem.at[t], col_rsem.at[t], peer))
        swap_col[t].start()
    bulk_x[1].start()
    bulk_y[1].start()
    with jax.named_scope("s16_relay_n_3_wait_recv_"):
        relay_n[3].wait_recv()
    with jax.named_scope("s17_relay_n_4_wait_recv_"):
        relay_n[4].wait_recv()
    with jax.named_scope("s18_partner_exps_ROWS_3_"):
        partner_exps(ROWS + 3 * CHUNK, CHUNK)
    with jax.named_scope("s19_swap_row_wait_recv_"):
        swap_row.wait_recv()
    row_tot = row_send[...] + jnp.concatenate([row_recv[:, ROWS:], row_recv[:, :ROWS]], axis=1)
    row_a = row_e
    row_l[...] = inv_count / row_tot
    swap_a = []
    for t, peer in enumerate(peers):
        swap_a.append(to_row(row_l, all_a.at[t], a_ssem.at[t], a_rsem.at[t], peer))
        swap_a[t].start()
    with jax.named_scope("s20_row_a_jnp_broadcast_"):
        row_a[...] = jnp.broadcast_to(row_l[...], (128, IMGS)).T
    for t in range(3):
        with jax.named_scope("s21_swap_col_t_wait_recv"):
            swap_col[t].wait_recv()
    def slot(ref, s):
        if s < 2:
            return ref[:, s * ROWS:(s + 1) * ROWS]
        starts = [X_BASE + (2 * p + s - 2) * PIECE for p in range(ROWS // PIECE)]
        return jnp.concatenate([ref[:, c:c + PIECE] for c in starts], axis=1)
    for s in range(4):
        tot = (slot(col_send, s) + slot(col_recv.at[0], s ^ 1)) + (slot(col_recv.at[1], s ^ 2) + slot(col_recv.at[2], s ^ 3))
        inverse = inv_count / tot
        if s < 2:
            col_b[:, s * ROWS:(s + 1) * ROWS] = inverse
        else:
            for p in range(ROWS // PIECE):
                start = X_BASE + (2 * p + s - 2) * PIECE
                col_b[:, start:start + PIECE] = inverse[:, p * PIECE:(p + 1) * PIECE]

    def d_img_chunk(r0):
        rows = pl.ds(r0, CHUNK)
        total = None
        for j in range(TXTS // 512):
            g = [exps[rows, c:c + 128] * (row_a[rows, :] + col_b[:, c:c + 128]) for c in range(j * 512, (j + 1) * 512, 128)]
            g = jnp.concatenate([v.astype(BF16) for v in g], axis=1)
            texts = txt[j // 2, j % 2 * 512:(j % 2 + 1) * 512, :] if j < 4 else far[2 * j - 8:2 * j - 6].reshape(512, DIM)
            part = jnp.dot(g, texts, preferred_element_type=F32)
            total = part if total is None else total + part
        return total

    def d_txt_chunk(starts):
        total = None
        for i in range(IMGS // 512):
            rows = slice(i * 512, (i + 1) * 512)
            g = []
            for start in starts:
                cols = pl.ds(start, PIECE)
                g.append((exps[rows, cols] * (row_a[rows, :] + col_b[:, cols])).astype(BF16))
            g = jnp.concatenate(g, axis=1)
            part = lax.dot_general(g, img[rows, :], (((0,), (0,)), ((), ())), preferred_element_type=F32)
            total = part if total is None else total + part
        return total

    swap_b = to_y(col_b, all_b, b_sem.at[0], b_sem.at[1])
    swap_b.start()
    own_r = row_send[:, :ROWS] + row_recv[:, ROWS:]
    loss_part = jnp.sum(jnp.log(own_r) - jnp.log(col_b[:, :ROWS] / inv_count)) - 2.0 * scale * diag_sum
    dscale_part = scale * (jnp.sum(row_a[...] * row_m[...]) + jnp.sum(jnp.sum(col_m[...], axis=0, keepdims=True) * col_b[...])
                           - 2.0 * inv_count * diag_sum)
    lane = lax.broadcasted_iota(jnp.int32, (8, 128), 1)
    scal[0] = jnp.where(lane == 0, loss_part * inv_count, dscale_part)
    send_s = [to_row(scal.at[0], scal.at[t + 1], sc_ssem.at[t], sc_rsem.at[t], peer) for t, peer in enumerate(peers)]
    for t in range(3):
        send_s[t].start()
    for k in range(2, BULK):
        bulk_x[k].start()
        bulk_y[k].start()

    corner = IMGS + ROWS
    d_img_acc = exps.at[pl.ds(ROWS, ROWS), pl.ds(corner, DIM)]
    d_txt_acc = exps.at[pl.ds(ROWS, ROWS), pl.ds(corner + DIM, DIM)]

    def fix_body(i, carry):
        part = pl.ds(pl.multiple_of(i * 128, 128), 128)
        on_diag = lax.broadcasted_iota(jnp.int32, (128, 128), 0) == lax.broadcasted_iota(jnp.int32, (128, 128), 1)
        term = (2.0 * inv_count) / (row_a[part, :] + col_b[:, part])
        exps[part, part] = exps[part, part] - jnp.where(on_diag, term, 0.0)
        return carry
    with jax.named_scope("s22_lax_fori_loop_0_ROWS"):
        lax.fori_loop(0, ROWS // 128, fix_body, 0)
    txt_b[...] = jnp.broadcast_to(col_b[:, :ROWS], (128, ROWS)).T

    def tile_body(k, carry):
        first = pl.multiple_of(k * CHUNK, CHUNK)
        part = pl.ds(first, CHUNK)
        with jax.named_scope("s23_d_img_acc_part_d_img"):
            d_img_acc[part, :] = d_img_chunk(first)
        with jax.named_scope("s24_d_txt_acc_part_d_txt"):
            d_txt_acc[part, :] = d_txt_chunk((first, first + PIECE))
        return carry
    with jax.named_scope("s25_lax_fori_loop_0_STEP"):
        lax.fori_loop(0, STEPS, tile_body, 0)

    for t in range(3):
        with jax.named_scope("s26_swap_a_t_wait_recv_"):
            swap_a[t].wait_recv()
        with jax.named_scope("s27_send_s_t_wait_recv_"):
            send_s[t].wait_recv()
    with jax.named_scope("s28_swap_b_wait_recv_"):
        swap_b.wait_recv()
    direct_b = jnp.concatenate([slot(all_b, 0), slot(all_b, 2)], axis=1)
    relayed_b = jnp.concatenate([slot(all_b, 1), slot(all_b, 3)], axis=1)
    for k in range(BULK):
        src, dst, size = (PIECE * v for v in bulk_span(k))
        for to, direct, relayed in ((new_a, all_a[1], all_a[2]), (new_b, direct_b, relayed_b)):
            to[:, dst:dst + size] = direct[:, src:src + size]
            to[:, dst + size:dst + 2 * size] = relayed[:, src:src + size]
    scal_y[0] = (scal[0] + scal[1]) + (scal[2] + scal[3])
    swap_s = to_y(scal_y.at[0], scal_y.at[1], sc_ssem.at[3], sc_rsem.at[3])
    swap_s.start()

    def partner_body(k, carry):
        first = pl.multiple_of(k * CHUNK, CHUNK)
        part = pl.ds(first, CHUNK)
        low = pl.ds(ROWS + first, CHUNK)
        total = None
        for j in range(IMGS // 512):
            g = [exps[low, ROWS + c:ROWS + c + 128] * (txt_b[part, :] + all_a[0, :, c:c + 128]) for c in range(j * 512, (j + 1) * 512, 128)]
            g = jnp.concatenate([v.astype(BF16) for v in g], axis=1)
            more = jnp.dot(g, img_p[j * 512:(j + 1) * 512, :], preferred_element_type=F32)
            total = more if total is None else total + more
        d_txt_acc[part, :] += total
        return carry
    with jax.named_scope("s29_lax_fori_loop_0_STEP"):
        lax.fori_loop(0, STEPS, partner_body, 0)

    def outside(own, own_factor, others, factor, total):
        dots = lax.dot_general(own, others, (((1,), (1,)), ((), ())), preferred_element_type=F32)
        e = jnp.exp2(dots * scale2)
        g = [(e[:, c:c + 128] * (own_factor + factor[:, c:c + 128])).astype(BF16) for c in range(0, others.shape[0], 128)]
        total[...] += jnp.dot(jnp.concatenate(g, axis=1), others, preferred_element_type=F32)

    def both_sides(start, size):
        part = pl.ds(start, size)
        outside(txt[0], txt_b[...], new_img[part, :], new_a[:, part], d_txt_acc)
        outside(img[0:ROWS, :], row_a[0:ROWS, :], new_txt[part, :], new_b[:, part], d_img_acc)

    def relays(k, dst, size):
        direct, relayed = pl.ds(dst, size), pl.ds(dst + size, size)
        rx = to_row(new_img_pieces.at[direct], new_img_pieces.at[relayed], fx_send.at[k], fx_recv.at[k], partner)
        ry = to_row(new_txt_pieces.at[direct], new_txt_pieces.at[relayed], fy_send.at[k], fy_recv.at[k], partner)
        return rx, ry

    def land(k, dst, size):
        direct = pl.ds(dst, size)
        rx, ry = relays(k, dst, size)
        to_row(new_img_pieces.at[direct], new_img_pieces.at[direct], bx_send.at[k], bx_recv.at[k], across).wait_recv()
        rx.start()
        to_y(new_txt_pieces.at[direct], new_txt_pieces.at[direct], by_send.at[k], by_recv.at[k]).wait_recv()
        ry.start()

    def relayed_in(k, dst, size):
        for copy in relays(k, dst, size):
            copy.wait_recv()

    with jax.named_scope("s30_land_0_0_2_"):
        land(0, 0, 2)
    with jax.named_scope("s31_both_sides_0_CHUNK_"):
        both_sides(0, CHUNK)

    def bulk_body(k, carry):
        with jax.named_scope("s32_land_k_4_k_2_"):
            land(k, 4 * k, 2)
        with jax.named_scope("s33_relayed_in_k_1_4_k_4"):
            relayed_in(k - 1, 4 * k - 4, 2)
        with jax.named_scope("s34_both_sides_pl_multip"):
            both_sides(pl.multiple_of(2 * k * CHUNK - CHUNK, CHUNK), 2 * CHUNK)
        return carry
    lax.fori_loop(1, WHOLE, bulk_body, 0)

    last = 2 * WHOLE * CHUNK
    with jax.named_scope("s35_relayed_in_WHOLE_1_4"):
        relayed_in(WHOLE - 1, 4 * WHOLE - 4, 2)
    with jax.named_scope("s36_both_sides_last_CHUN"):
        both_sides(last - CHUNK, CHUNK)
    with jax.named_scope("s37_land_WHOLE_4_WHOLE_1"):
        land(WHOLE, 4 * WHOLE, 1)
    with jax.named_scope("s38_both_sides_last_PIEC"):
        both_sides(last, PIECE)
    with jax.named_scope("s39_relayed_in_WHOLE_4_W"):
        relayed_in(WHOLE, 4 * WHOLE, 1)
    with jax.named_scope("s40_both_sides_last_PIEC"):
        both_sides(last + PIECE, PIECE)
    with jax.named_scope("s41_land_WHOLE_1_4_WHOLE"):
        land(WHOLE + 1, 4 * WHOLE + 2, 1)
    with jax.named_scope("s42_both_sides_last_2_PI"):
        both_sides(last + 2 * PIECE, PIECE)
    with jax.named_scope("s43_relayed_in_WHOLE_1_4"):
        relayed_in(WHOLE + 1, 4 * WHOLE + 2, 1)
    with jax.named_scope("s44_both_sides_last_3_PI"):
        both_sides(last + 3 * PIECE, PIECE)

    with jax.named_scope("s45_dimg_ref_scale_d_img"):
        dimg_ref[...] = (scale * d_img_acc[...]).astype(BF16)
    dtxt_ref[...] = (scale * d_txt_acc[...]).astype(BF16)

    with jax.named_scope("s46_swap_s_wait_recv_"):
        swap_s.wait_recv()
    total = scal_y[0] + scal_y[1]
    loss_ref[0, 0] = total[0, 0]
    dscale_ref[0, 0] = total[0, 1]

    for k in range(G_STEPS):
        gather_x[k].wait_send()
        gather_y[k].wait_send()
        relay[k].wait_send()
        relay_n[k].wait_send()
    for k in range(BULK):
        bulk_x[k].wait_send()
        bulk_y[k].wait_send()
        src, dst, size = bulk_span(k)
        for copy in relays(k, dst, size):
            copy.wait_send()
    gather_p.wait_send()
    gather_i.wait_send()
    swap_b.wait_send()
    swap_row.wait_send()
    for t in range(3):
        swap_col[t].wait_send()
        send_s[t].wait_send()
        swap_a[t].wait_send()
    swap_s.wait_send()


def solution(mesh):
    batch_spec = P(("row", "col"), None)
    n_dev = mesh.shape["row"] * mesh.shape["col"]
    inv_count = 1.0 / (2 * ROWS * n_dev)
    dma = pltpu.SemaphoreType.DMA

    def local_tile(img_loc, txt_loc, log_scale):
        any_spec = pl.BlockSpec(memory_space=pl.ANY)
        vmem_spec = pl.BlockSpec(memory_space=pltpu.VMEM)
        smem_spec = pl.BlockSpec(memory_space=pltpu.SMEM)
        loss, d_img, d_txt, d_scale = pl.pallas_call(
            functools.partial(kernel, inv_count),
            out_shape=(
                jax.ShapeDtypeStruct((1, 1), F32),
                pltpu.VMEM((ROWS, DIM), BF16),
                pltpu.VMEM((ROWS, DIM), BF16),
                jax.ShapeDtypeStruct((1, 1), F32),
            ),
            in_specs=[smem_spec, any_spec, any_spec],
            out_specs=(smem_spec, vmem_spec, vmem_spec, smem_spec),
            scratch_shapes=[
                pltpu.VMEM((IMGS, DIM), BF16),
                pltpu.VMEM((2, ROWS, DIM), BF16),
                pltpu.VMEM((ROWS // PIECE, 2, PIECE, DIM), BF16),
                pltpu.VMEM((DIM, TXTS), BF16),
                pltpu.VMEM((IMGS, DIM), BF16),
                pltpu.VMEM((TXTS, DIM), BF16),
                pltpu.VMEM((TXTS, DIM), BF16),
                pltpu.VMEM((IMGS, TXTS), F32),
                pltpu.VMEM((IMGS, 128), F32),
                pltpu.VMEM((IMGS, 128), F32),
                pltpu.VMEM((8, TXTS), F32),
                pltpu.VMEM((8, TXTS), F32),
                pltpu.VMEM((1, IMGS), F32),
                pltpu.VMEM((1, IMGS), F32),
                pltpu.VMEM((1, TXTS), F32),
                pltpu.VMEM((3, 1, TXTS), F32),
                pltpu.VMEM((1, TXTS), F32),
                pltpu.VMEM((1, IMGS), F32),
                pltpu.VMEM((3, 1, IMGS), F32),
                pltpu.VMEM((1, TXTS), F32),
                pltpu.VMEM((1, TXTS), F32),
                pltpu.VMEM((1, TXTS), F32),
                pltpu.VMEM((ROWS, 128), F32),
                pltpu.VMEM((4, 8, 128), F32),
                pltpu.VMEM((2, 8, 128), F32),
                dma((2,)),
                dma((G_STEPS,)), dma((G_STEPS,)),
                dma((G_STEPS,)), dma((G_STEPS,)),
                dma((4,)),
                dma((G_STEPS,)), dma((G_STEPS,)),
                dma((2,)),
                dma((3,)), dma((3,)),
                dma((BULK,)), dma((BULK,)), dma((BULK,)), dma((BULK,)),
                dma((BULK,)), dma((BULK,)), dma((BULK,)), dma((BULK,)),
                dma((G_STEPS,)), dma((G_STEPS,)),
                dma((3,)), dma((3,)), dma((2,)),
                dma((4,)), dma((4,)),
            ],
            compiler_params=pltpu.CompilerParams(
                collective_id=0, has_side_effects=True, vmem_limit_bytes=VMEM_LIMIT,
            ),
            name="clip_loss",
        )(log_scale.reshape(1, 1), img_loc, txt_loc)
        return loss.reshape(()), d_img, d_txt, d_scale.reshape(())

    return jax.shard_map(local_tile, mesh=mesh, in_specs=(batch_spec, batch_spec, P()), out_specs=(P(), batch_spec, batch_spec, P()), check_vma=False)
```

```python
import functools
import math

import jax
import jax.numpy as jnp
from jax import lax
from jax.experimental import pallas as pl
from jax.experimental.pallas import tpu as pltpu
from jax.sharding import PartitionSpec as P

MESH = pl.DeviceIdType.MESH
VMEM_LIMIT = 247 * 256 * 1024
F32 = jnp.float32
BF16 = jnp.bfloat16
ROWS = 1024
DIM = 512
CHUNK = 256
STEPS = ROWS // CHUNK
SIZES = (2, 1, 2, 2, 2, 2, 2, 2, 1)
TXT_START = (0, 8, 2, 4, 6, 9, 11, 13, 15)
BULK = len(SIZES)
PIECE = 128
GATHER = (2, 2, 2, 1, 1)
G_START = tuple(sum(GATHER[:k]) for k in range(len(GATHER)))
G_STEPS = len(GATHER)
IMGS = 2 * ROWS
TXTS = 4 * ROWS
X_BASE = 2 * ROWS
LOG2E = math.log2(math.e)


def kernel(inv_count, scale_ref, img_hbm, txt_hbm, loss_ref, dimg_ref, dtxt_ref, dscale_ref,
           img, txt, far, txt_t, img_p, new_txt, new_img, exps, row_e, row_m, col_e, col_m, row_send, row_recv, col_send, col_recv, col_b, row_l, all_a, all_b, new_a, new_b, txt_b,
           scal, scal_y, load_sem, gy_send, gy_recv, gx_send, gx_recv, gp_sem, gf_send, gf_recv, row_sem, col_ssem, col_rsem,
           bx_send, bx_recv, by_send, by_recv, fx_send, fx_recv, fy_send, fy_recv, pn_send, pn_recv,
           a_ssem, a_rsem, b_sem, sc_ssem, sc_rsem):
    row = lax.axis_index("row")
    col = lax.axis_index("col")
    core = lax.rem(row, 2)
    partner = row + 1 - 2 * core
    across = lax.rem(row + 2, 4)
    diagonal = across + 1 - 2 * core
    peers = (partner, across, diagonal)
    other_col = 1 - col

    def to_y(src, dst, ssem, rsem):
        return pltpu.make_async_remote_copy(src, dst, ssem, rsem, device_id={"row": row, "col": other_col}, device_id_type=MESH)

    def to_row(src, dst, ssem, rsem, peer):
        return pltpu.make_async_remote_copy(src, dst, ssem, rsem, device_id={"row": peer, "col": col}, device_id_type=MESH)

    txt_pieces = txt.at[0].reshape(ROWS // PIECE, PIECE, DIM)
    loads = []
    for k in range(G_STEPS):
        part = pl.ds(G_START[k] * PIECE, GATHER[k] * PIECE)
        loads.append((pltpu.make_async_copy(txt_hbm.at[part], txt.at[0, part], load_sem.at[k]),
                      pltpu.make_async_copy(img_hbm.at[part], img.at[part], load_sem.at[G_STEPS + k])))
        for copy in loads[k]:
            copy.start()

    barrier = pltpu.get_barrier_semaphore()
    for peer in peers:
        pl.semaphore_signal(barrier, inc=1, device_id={"row": peer, "col": col}, device_id_type=MESH)
    pl.semaphore_signal(barrier, inc=1, device_id={"row": row, "col": other_col}, device_id_type=MESH)

    pl.semaphore_wait(barrier, 4)

    gather_y, gather_x, relay = [], [], []
    for k in range(G_STEPS):
        pieces = pl.ds(G_START[k], GATHER[k])
        part = pl.ds(G_START[k] * PIECE, GATHER[k] * PIECE)
        gather_x.append(to_row(txt_pieces.at[pieces], far.at[pieces, 0], gx_send.at[k], gx_recv.at[k], across))
        gather_y.append(to_y(img.at[part], img.at[pl.ds(ROWS + G_START[k] * PIECE, GATHER[k] * PIECE)], gy_send.at[k], gy_recv.at[k]))
        relay.append(to_row(far.at[pieces, 0], far.at[pieces, 1], gf_send.at[k], gf_recv.at[k], partner))
        loads[k][0].wait()
        gather_x[k].start()
        loads[k][1].wait()
        gather_y[k].start()
    gather_p = to_row(txt.at[0], txt.at[1], gp_sem.at[0], gp_sem.at[1], partner)
    gather_p.start()
    gather_i = to_row(img.at[pl.ds(0, ROWS)], img_p.at[pl.ds(0, ROWS)], gp_sem.at[2], gp_sem.at[3], partner)
    gather_i.start()
    relay_n = []
    for k in range(G_STEPS):
        part = pl.ds(ROWS + G_START[k] * PIECE, GATHER[k] * PIECE)
        relay_n.append(to_row(img.at[part], img_p.at[part], pn_send.at[k], pn_recv.at[k], partner))

    img_pieces = img.reshape(IMGS // PIECE, PIECE, DIM)
    new_img_pieces = new_img.reshape(TXTS // PIECE, PIECE, DIM)
    new_txt_pieces = new_txt.reshape(TXTS // PIECE, PIECE, DIM)

    def bulk_span(k):
        start = sum(SIZES[:k])
        return start, 2 * start, SIZES[k]

    bulk_x, bulk_y = [], []
    for k in range(BULK):
        src, dst, size = bulk_span(k)
        land = pl.ds(dst, size)
        bulk_x.append(to_row(img_pieces.at[pl.ds(src, size)], new_img_pieces.at[land], bx_send.at[k], bx_recv.at[k], across))
        half = ROWS // PIECE
        src = TXT_START[k]
        source = txt_pieces.at[pl.ds(src, size)] if src < half else far.at[pl.ds(src - half, size), 0]
        bulk_y.append(to_y(source, new_txt_pieces.at[land], by_send.at[k], by_recv.at[k]))
    bulk_x[0].start()
    bulk_y[0].start()
    bulk_x[1].start()

    scale = jnp.max(jnp.exp(jnp.full((8, 128), scale_ref[0, 0], F32)))
    scale2 = scale * LOG2E
    row_e[...] = jnp.zeros_like(row_e)
    row_m[...] = jnp.zeros_like(row_m)
    col_e[...] = jnp.zeros_like(col_e)
    col_m[...] = jnp.zeros_like(col_m)

    def logit_block(r0, nr, c0, nc, texts, on_rows, kept):
        rows = pl.ds(r0, nr)
        cols = pl.ds(c0, nc)
        dots = lax.dot_general(img[rows, :], texts, (((1,), (1 if on_rows else 0,)), ((), ())), preferred_element_type=F32)
        e = jnp.exp2(dots * scale2)
        if kept:
            exps[pl.ds(r0, kept), cols] = e[:kept]
        m = e * dots
        for values, row_sum, col_sum in ((e, row_e, col_e), (m, row_m, col_m)):
            acc = values[:, 0:128]
            for q in range(1, nc // 128):
                acc = acc + values[:, q * 128:(q + 1) * 128]
            row_sum[rows, :] += acc
            col_sum[:, cols] += jnp.sum(values.reshape(nr // 8, 8, nc), axis=0)

    def own_by_held(slot):
        def body(i, carry):
            part = pl.ds(pl.multiple_of(i * 512, 512), 512)
            logit_block(0, ROWS, pl.multiple_of(slot * ROWS + i * 512, 512), 512, txt[slot, part, :], True, ROWS)
            return carry
        lax.fori_loop(0, 2, body, 0)

    def turn_held(slot):
        def body(i, carry):
            part = pl.ds(pl.multiple_of(i * CHUNK, CHUNK), CHUNK)
            txt_t[:, pl.ds(pl.multiple_of(slot * ROWS + i * CHUNK, CHUNK), CHUNK)] = txt[slot, part, :].T
            return carry
        lax.fori_loop(0, STEPS, body, 0)

    def partner_exps(c0, n):
        dots = lax.dot_general(txt[0], img_p[pl.ds(c0, n), :], (((1,), (1,)), ((), ())), preferred_element_type=F32)
        exps[ROWS:, pl.ds(ROWS + c0, n)] = jnp.exp2(dots * scale2)

    own_by_held(0)
    turn_held(0)

    def diag_body(i, acc):
        part = pl.ds(pl.multiple_of(i * 128, 128), 128)
        prod = img[part, :].astype(F32) * txt[0, part, :].astype(F32)
        return acc + jnp.sum(prod.reshape(16, 8, DIM), axis=0)
    diag_sum = jnp.sum(lax.fori_loop(0, 8, diag_body, jnp.zeros((8, DIM), F32)))

    gather_p.wait_recv()
    own_by_held(1)
    turn_held(1)
    gather_i.wait_recv()
    def partner_own(i, carry):
        partner_exps(pl.multiple_of(i * 512, 512), 512)
        return carry
    lax.fori_loop(0, 2, partner_own, 0)
    for k in range(G_STEPS):
        n_rows = GATHER[k] * PIECE
        done = G_START[k] * PIECE
        new_row = ROWS + done
        gather_x[k].wait_recv()
        relay[k].start()
        if k == 0:
            bulk_y[1].start()
        gather_y[k].wait_recv()
        relay_n[k].start()
        def new_by_held(i, carry, new_row=new_row, n_rows=n_rows):
            c0 = pl.multiple_of(i * 1024, 1024)
            logit_block(new_row, n_rows, c0, 1024, txt_t[:, pl.ds(c0, 1024)], False, 0)
            return carry
        n_held = X_BASE + 2 * done
        logit_block(new_row, n_rows, 0, ROWS, txt_t[:, :ROWS], False, n_rows)
        lax.fori_loop(1, n_held // 1024, new_by_held, 0)
        if n_held % 1024:
            c0 = n_held // 1024 * 1024
            logit_block(new_row, n_rows, c0, n_held - c0, txt_t[:, c0:n_held], False, 0)
        relay[k].wait_recv()
        new_cols = 2 * n_rows
        logit_block(0, new_row + n_rows, n_held, new_cols, far[G_START[k]:G_START[k] + GATHER[k]].reshape(new_cols, DIM), True, ROWS)
        if k + 1 < G_STEPS:
            for p in range(G_START[k], G_START[k] + GATHER[k]):
                c0 = X_BASE + 2 * p * PIECE
                txt_t[:, c0:c0 + 2 * PIECE] = far[p].reshape(2 * PIECE, DIM).T
        if k < 3:
            relay_n[k].wait_recv()
            partner_exps(ROWS + k * CHUNK, CHUNK)

    row_send[...] = jnp.sum(row_e[...].T, axis=0, keepdims=True)
    col_send[...] = jnp.sum(col_e[...], axis=0, keepdims=True)
    swap_row = to_y(row_send, row_recv, row_sem.at[0], row_sem.at[1])
    swap_row.start()
    swap_col = []
    for t, peer in enumerate(peers):
        swap_col.append(to_row(col_send, col_recv.at[t], col_ssem.at[t], col_rsem.at[t], peer))
        swap_col[t].start()
    bulk_x[2].start()
    bulk_y[2].start()
    relay_n[3].wait_recv()
    relay_n[4].wait_recv()
    partner_exps(ROWS + 3 * CHUNK, CHUNK)
    swap_row.wait_recv()
    row_tot = row_send[...] + jnp.concatenate([row_recv[:, ROWS:], row_recv[:, :ROWS]], axis=1)
    row_a = row_e
    row_l[...] = inv_count / row_tot
    swap_a = []
    for t, peer in enumerate(peers):
        swap_a.append(to_row(row_l, all_a.at[t], a_ssem.at[t], a_rsem.at[t], peer))
        swap_a[t].start()
    row_a[...] = jnp.broadcast_to(row_l[...], (128, IMGS)).T
    for t in range(3):
        swap_col[t].wait_recv()
    def slot(ref, s):
        if s < 2:
            return ref[:, s * ROWS:(s + 1) * ROWS]
        starts = [X_BASE + (2 * p + s - 2) * PIECE for p in range(ROWS // PIECE)]
        return jnp.concatenate([ref[:, c:c + PIECE] for c in starts], axis=1)
    for s in range(4):
        tot = (slot(col_send, s) + slot(col_recv.at[0], s ^ 1)) + (slot(col_recv.at[1], s ^ 2) + slot(col_recv.at[2], s ^ 3))
        inverse = inv_count / tot
        if s < 2:
            col_b[:, s * ROWS:(s + 1) * ROWS] = inverse
        else:
            for p in range(ROWS // PIECE):
                start = X_BASE + (2 * p + s - 2) * PIECE
                col_b[:, start:start + PIECE] = inverse[:, p * PIECE:(p + 1) * PIECE]

    def d_img_chunk(r0):
        rows = pl.ds(r0, CHUNK)
        total = None
        for j in range(TXTS // 512):
            g = [exps[rows, c:c + 128] * (row_a[rows, :] + col_b[:, c:c + 128]) for c in range(j * 512, (j + 1) * 512, 128)]
            g = jnp.concatenate([v.astype(BF16) for v in g], axis=1)
            texts = txt[j // 2, j % 2 * 512:(j % 2 + 1) * 512, :] if j < 4 else far[2 * j - 8:2 * j - 6].reshape(512, DIM)
            part = jnp.dot(g, texts, preferred_element_type=F32)
            total = part if total is None else total + part
        return total

    def d_txt_chunk(starts):
        total = None
        for i in range(IMGS // 512):
            rows = slice(i * 512, (i + 1) * 512)
            g = []
            for start in starts:
                cols = pl.ds(start, PIECE)
                g.append((exps[rows, cols] * (row_a[rows, :] + col_b[:, cols])).astype(BF16))
            g = jnp.concatenate(g, axis=1)
            part = lax.dot_general(g, img[rows, :], (((0,), (0,)), ((), ())), preferred_element_type=F32)
            total = part if total is None else total + part
        return total

    swap_b = to_y(col_b, all_b, b_sem.at[0], b_sem.at[1])
    swap_b.start()
    own_r = row_send[:, :ROWS] + row_recv[:, ROWS:]
    loss_part = jnp.sum(jnp.log(own_r) - jnp.log(col_b[:, :ROWS] / inv_count)) - 2.0 * scale * diag_sum
    dscale_part = scale * (jnp.sum(row_a[...] * row_m[...]) + jnp.sum(jnp.sum(col_m[...], axis=0, keepdims=True) * col_b[...])
                           - 2.0 * inv_count * diag_sum)
    lane = lax.broadcasted_iota(jnp.int32, (8, 128), 1)
    scal[0] = jnp.where(lane == 0, loss_part * inv_count, dscale_part)
    send_s = [to_row(scal.at[0], scal.at[t + 1], sc_ssem.at[t], sc_rsem.at[t], peer) for t, peer in enumerate(peers)]
    for t in range(3):
        send_s[t].start()
    for k in range(3, BULK):
        bulk_x[k].start()
        bulk_y[k].start()

    corner = IMGS + ROWS
    d_img_acc = exps.at[pl.ds(ROWS, ROWS), pl.ds(corner, DIM)]
    d_txt_acc = exps.at[pl.ds(ROWS, ROWS), pl.ds(corner + DIM, DIM)]

    def fix_body(i, carry):
        part = pl.ds(pl.multiple_of(i * 128, 128), 128)
        on_diag = lax.broadcasted_iota(jnp.int32, (128, 128), 0) == lax.broadcasted_iota(jnp.int32, (128, 128), 1)
        term = (2.0 * inv_count) / (row_a[part, :] + col_b[:, part])
        exps[part, part] = exps[part, part] - jnp.where(on_diag, term, 0.0)
        return carry
    lax.fori_loop(0, ROWS // 128, fix_body, 0)
    txt_b[...] = jnp.broadcast_to(col_b[:, :ROWS], (128, ROWS)).T

    def tile_body(k, carry):
        first = pl.multiple_of(k * CHUNK, CHUNK)
        part = pl.ds(first, CHUNK)
        d_img_acc[part, :] = d_img_chunk(first)
        d_txt_acc[part, :] = d_txt_chunk((first, first + PIECE))
        return carry
    lax.fori_loop(0, STEPS, tile_body, 0)

    for t in range(3):
        swap_a[t].wait_recv()
        send_s[t].wait_recv()
    swap_b.wait_recv()
    direct_b = jnp.concatenate([slot(all_b, 0), slot(all_b, 2)], axis=1)
    relayed_b = jnp.concatenate([slot(all_b, 1), slot(all_b, 3)], axis=1)
    for k in range(BULK):
        src_a, dst, size = (PIECE * v for v in bulk_span(k))
        src_b = PIECE * TXT_START[k]
        for to, direct, relayed, src in ((new_a, all_a[1], all_a[2], src_a), (new_b, direct_b, relayed_b, src_b)):
            to[:, dst:dst + size] = direct[:, src:src + size]
            to[:, dst + size:dst + 2 * size] = relayed[:, src:src + size]
    scal_y[0] = (scal[0] + scal[1]) + (scal[2] + scal[3])
    swap_s = to_y(scal_y.at[0], scal_y.at[1], sc_ssem.at[3], sc_rsem.at[3])
    swap_s.start()

    def partner_body(k, carry):
        first = pl.multiple_of(k * CHUNK, CHUNK)
        part = pl.ds(first, CHUNK)
        low = pl.ds(ROWS + first, CHUNK)
        total = None
        for j in range(IMGS // 512):
            g = [exps[low, ROWS + c:ROWS + c + 128] * (txt_b[part, :] + all_a[0, :, c:c + 128]) for c in range(j * 512, (j + 1) * 512, 128)]
            g = jnp.concatenate([v.astype(BF16) for v in g], axis=1)
            more = jnp.dot(g, img_p[j * 512:(j + 1) * 512, :], preferred_element_type=F32)
            total = more if total is None else total + more
        d_txt_acc[part, :] += total
        return carry
    lax.fori_loop(0, STEPS, partner_body, 0)

    def outside(own, own_factor, others, factor, total):
        dots = lax.dot_general(own, others, (((1,), (1,)), ((), ())), preferred_element_type=F32)
        e = jnp.exp2(dots * scale2)
        g = [(e[:, c:c + 128] * (own_factor + factor[:, c:c + 128])).astype(BF16) for c in range(0, others.shape[0], 128)]
        total[...] += jnp.dot(jnp.concatenate(g, axis=1), others, preferred_element_type=F32)

    def both_sides(start, size):
        part = pl.ds(start, size)
        outside(txt[0], txt_b[...], new_img[part, :], new_a[:, part], d_txt_acc)
        outside(img[0:ROWS, :], row_a[0:ROWS, :], new_txt[part, :], new_b[:, part], d_img_acc)

    def relays(k, dst, size):
        direct, relayed = pl.ds(dst, size), pl.ds(dst + size, size)
        rx = to_row(new_img_pieces.at[direct], new_img_pieces.at[relayed], fx_send.at[k], fx_recv.at[k], partner)
        ry = to_row(new_txt_pieces.at[direct], new_txt_pieces.at[relayed], fy_send.at[k], fy_recv.at[k], partner)
        return rx, ry

    def land(k, dst, size):
        direct = pl.ds(dst, size)
        rx, ry = relays(k, dst, size)
        to_row(new_img_pieces.at[direct], new_img_pieces.at[direct], bx_send.at[k], bx_recv.at[k], across).wait_recv()
        rx.start()
        to_y(new_txt_pieces.at[direct], new_txt_pieces.at[direct], by_send.at[k], by_recv.at[k]).wait_recv()
        ry.start()

    def relayed_in(k, dst, size):
        for copy in relays(k, dst, size):
            copy.wait_recv()

    def sent(k, dst, size):
        direct = pl.ds(dst, size)
        to_row(new_img_pieces.at[direct], new_img_pieces.at[direct], bx_send.at[k], bx_recv.at[k], across).wait_send()
        to_y(new_txt_pieces.at[direct], new_txt_pieces.at[direct], by_send.at[k], by_recv.at[k]).wait_send()
        for copy in relays(k, dst, size):
            copy.wait_send()

    def early_sent():
        for k in range(G_STEPS):
            gather_x[k].wait_send()
            gather_y[k].wait_send()
            relay[k].wait_send()
            relay_n[k].wait_send()
        for k in range(2):
            sent(k, *bulk_span(k)[1:])
        gather_p.wait_send()
        gather_i.wait_send()
        swap_b.wait_send()
        swap_row.wait_send()
        for t in range(3):
            swap_col[t].wait_send()
            send_s[t].wait_send()
            swap_a[t].wait_send()

    land(0, 0, 2)
    both_sides(0, CHUNK)
    land(1, 4, 1)
    relayed_in(0, 0, 2)
    both_sides(CHUNK, CHUNK + PIECE)
    land(2, 6, 2)
    relayed_in(1, 4, 1)
    both_sides(2 * CHUNK + PIECE, CHUNK + PIECE)

    def bulk_body(k, carry):
        @pl.when(k == 5)
        def _():
            early_sent()
        land(k, 4 * k - 2, 2)
        relayed_in(k - 1, 4 * k - 6, 2)
        sent(k - 1, 4 * k - 6, 2)
        both_sides(pl.multiple_of(2 * (k - 1) * CHUNK, CHUNK), 2 * CHUNK)
        return carry
    lax.fori_loop(3, BULK - 1, bulk_body, 0)

    src, dst, size = bulk_span(BULK - 1)
    land(BULK - 1, dst, size)
    relayed_in(BULK - 2, dst - 4, 2)
    both_sides(dst * PIECE - CHUNK, CHUNK + PIECE)
    relayed_in(BULK - 1, dst, size)
    both_sides((dst + 1) * PIECE, PIECE)

    dimg_ref[...] = (scale * d_img_acc[...]).astype(BF16)
    dtxt_ref[...] = (scale * d_txt_acc[...]).astype(BF16)

    swap_s.wait_recv()
    total = scal_y[0] + scal_y[1]
    loss_ref[0, 0] = total[0, 0]
    dscale_ref[0, 0] = total[0, 1]

    for k in range(BULK - 2, BULK):
        sent(k, *bulk_span(k)[1:])
    swap_s.wait_send()


def solution(mesh):
    batch_spec = P(("row", "col"), None)
    n_dev = mesh.shape["row"] * mesh.shape["col"]
    inv_count = 1.0 / (2 * ROWS * n_dev)
    dma = pltpu.SemaphoreType.DMA

    def local_tile(img_loc, txt_loc, log_scale):
        any_spec = pl.BlockSpec(memory_space=pl.ANY)
        vmem_spec = pl.BlockSpec(memory_space=pltpu.VMEM)
        smem_spec = pl.BlockSpec(memory_space=pltpu.SMEM)
        loss, d_img, d_txt, d_scale = pl.pallas_call(
            functools.partial(kernel, inv_count),
            out_shape=(
                jax.ShapeDtypeStruct((1, 1), F32),
                pltpu.VMEM((ROWS, DIM), BF16),
                pltpu.VMEM((ROWS, DIM), BF16),
                jax.ShapeDtypeStruct((1, 1), F32),
            ),
            in_specs=[smem_spec, any_spec, any_spec],
            out_specs=(smem_spec, vmem_spec, vmem_spec, smem_spec),
            scratch_shapes=[
                pltpu.VMEM((IMGS, DIM), BF16),
                pltpu.VMEM((2, ROWS, DIM), BF16),
                pltpu.VMEM((ROWS // PIECE, 2, PIECE, DIM), BF16),
                pltpu.VMEM((DIM, TXTS), BF16),
                pltpu.VMEM((IMGS, DIM), BF16),
                pltpu.VMEM((TXTS, DIM), BF16),
                pltpu.VMEM((TXTS, DIM), BF16),
                pltpu.VMEM((IMGS, TXTS), F32),
                pltpu.VMEM((IMGS, 128), F32),
                pltpu.VMEM((IMGS, 128), F32),
                pltpu.VMEM((8, TXTS), F32),
                pltpu.VMEM((8, TXTS), F32),
                pltpu.VMEM((1, IMGS), F32),
                pltpu.VMEM((1, IMGS), F32),
                pltpu.VMEM((1, TXTS), F32),
                pltpu.VMEM((3, 1, TXTS), F32),
                pltpu.VMEM((1, TXTS), F32),
                pltpu.VMEM((1, IMGS), F32),
                pltpu.VMEM((3, 1, IMGS), F32),
                pltpu.VMEM((1, TXTS), F32),
                pltpu.VMEM((1, TXTS), F32),
                pltpu.VMEM((1, TXTS), F32),
                pltpu.VMEM((ROWS, 128), F32),
                pltpu.VMEM((4, 8, 128), F32),
                pltpu.VMEM((2, 8, 128), F32),
                dma((2 * G_STEPS,)),
                dma((G_STEPS,)), dma((G_STEPS,)),
                dma((G_STEPS,)), dma((G_STEPS,)),
                dma((4,)),
                dma((G_STEPS,)), dma((G_STEPS,)),
                dma((2,)),
                dma((3,)), dma((3,)),
                dma((BULK,)), dma((BULK,)), dma((BULK,)), dma((BULK,)),
                dma((BULK,)), dma((BULK,)), dma((BULK,)), dma((BULK,)),
                dma((G_STEPS,)), dma((G_STEPS,)),
                dma((3,)), dma((3,)), dma((2,)),
                dma((4,)), dma((4,)),
            ],
            compiler_params=pltpu.CompilerParams(
                collective_id=0, has_side_effects=True, vmem_limit_bytes=VMEM_LIMIT,
            ),
            name="clip_loss",
        )(log_scale.reshape(1, 1), img_loc, txt_loc)
        return loss.reshape(()), d_img, d_txt, d_scale.reshape(())

    return jax.shard_map(local_tile, mesh=mesh, in_specs=(batch_spec, batch_spec, P()), out_specs=(P(), batch_spec, batch_spec, P()), check_vma=False)
```

```python
import functools
import math

import jax
import jax.numpy as jnp
from jax import lax
from jax.experimental import pallas as pl
from jax.experimental.pallas import tpu as pltpu
from jax.sharding import PartitionSpec as P

MESH = pl.DeviceIdType.MESH
VMEM_LIMIT = 247 * 256 * 1024
MARGIN = 4 * 1024 * 1024
F32 = jnp.float32
BF16 = jnp.bfloat16
ROWS = 1024
DIM = 512
CHUNK = 256
STEPS = ROWS // CHUNK
SIZES = (2, 1, 2, 2, 2, 2, 2, 2, 1)
TXT_START = (0, 8, 2, 4, 6, 9, 11, 13, 15)
BULK = len(SIZES)
PIECE = 128
GATHER = (2, 2, 2, 1, 1)
G_START = tuple(sum(GATHER[:k]) for k in range(len(GATHER)))
G_STEPS = len(GATHER)
IMGS = 2 * ROWS
TXTS = 4 * ROWS
X_BASE = 2 * ROWS
LOG2E = math.log2(math.e)


def kernel(inv_count, scale_ref, img_hbm, txt_hbm, loss_ref, dimg_ref, dtxt_ref, dscale_ref,
           img, txt, far, txt_t, img_p, new_txt, new_img, exps, row_e, row_m, col_e, col_m, row_send, row_recv, col_send, col_recv, col_b, row_l, all_a, all_b, new_a, new_b, txt_b,
           scal, scal_y, load_sem, gy_send, gy_recv, gx_send, gx_recv, gp_sem, gf_send, gf_recv, row_sem, col_ssem, col_rsem,
           bx_send, bx_recv, by_send, by_recv, fx_send, fx_recv, fy_send, fy_recv, pn_send, pn_recv,
           a_ssem, a_rsem, b_sem, sc_ssem, sc_rsem):
    row = lax.axis_index("row")
    col = lax.axis_index("col")
    core = lax.rem(row, 2)
    partner = row + 1 - 2 * core
    across = lax.rem(row + 2, 4)
    diagonal = across + 1 - 2 * core
    peers = (partner, across, diagonal)
    other_col = 1 - col

    def to_y(src, dst, ssem, rsem):
        return pltpu.make_async_remote_copy(src, dst, ssem, rsem, device_id={"row": row, "col": other_col}, device_id_type=MESH)

    def to_row(src, dst, ssem, rsem, peer):
        return pltpu.make_async_remote_copy(src, dst, ssem, rsem, device_id={"row": peer, "col": col}, device_id_type=MESH)

    txt_pieces = txt.at[0].reshape(ROWS // PIECE, PIECE, DIM)
    loads = []
    for k in range(G_STEPS):
        part = pl.ds(G_START[k] * PIECE, GATHER[k] * PIECE)
        loads.append((pltpu.make_async_copy(txt_hbm.at[part], txt.at[0, part], load_sem.at[k]),
                      pltpu.make_async_copy(img_hbm.at[part], img.at[part], load_sem.at[G_STEPS + k])))
        for copy in loads[k]:
            copy.start()

    barrier = pltpu.get_barrier_semaphore()
    for peer in peers:
        pl.semaphore_signal(barrier, inc=1, device_id={"row": peer, "col": col}, device_id_type=MESH)
    pl.semaphore_signal(barrier, inc=1, device_id={"row": row, "col": other_col}, device_id_type=MESH)

    with jax.named_scope("p1"):
        pl.semaphore_wait(barrier, 4)

    gather_y, gather_x, relay = [], [], []
    for k in range(G_STEPS):
        pieces = pl.ds(G_START[k], GATHER[k])
        part = pl.ds(G_START[k] * PIECE, GATHER[k] * PIECE)
        gather_x.append(to_row(txt_pieces.at[pieces], far.at[pieces, 0], gx_send.at[k], gx_recv.at[k], across))
        gather_y.append(to_y(img.at[part], img.at[pl.ds(ROWS + G_START[k] * PIECE, GATHER[k] * PIECE)], gy_send.at[k], gy_recv.at[k]))
        relay.append(to_row(far.at[pieces, 0], far.at[pieces, 1], gf_send.at[k], gf_recv.at[k], partner))
        loads[k][0].wait()
        gather_x[k].start()
        loads[k][1].wait()
        gather_y[k].start()
    gather_p = to_row(txt.at[0], txt.at[1], gp_sem.at[0], gp_sem.at[1], partner)
    gather_p.start()
    gather_i = to_row(img.at[pl.ds(0, ROWS)], img_p.at[pl.ds(0, ROWS)], gp_sem.at[2], gp_sem.at[3], partner)
    gather_i.start()
    relay_n = []
    for k in range(G_STEPS):
        part = pl.ds(ROWS + G_START[k] * PIECE, GATHER[k] * PIECE)
        relay_n.append(to_row(img.at[part], img_p.at[part], pn_send.at[k], pn_recv.at[k], partner))

    img_pieces = img.reshape(IMGS // PIECE, PIECE, DIM)
    new_img_pieces = new_img.reshape(TXTS // PIECE, PIECE, DIM)
    new_txt_pieces = new_txt.reshape(TXTS // PIECE, PIECE, DIM)

    def bulk_span(k):
        start = sum(SIZES[:k])
        return start, 2 * start, SIZES[k]

    bulk_x, bulk_y = [], []
    for k in range(BULK):
        src, dst, size = bulk_span(k)
        land = pl.ds(dst, size)
        bulk_x.append(to_row(img_pieces.at[pl.ds(src, size)], new_img_pieces.at[land], bx_send.at[k], bx_recv.at[k], across))
        half = ROWS // PIECE
        src = TXT_START[k]
        source = txt_pieces.at[pl.ds(src, size)] if src < half else far.at[pl.ds(src - half, size), 0]
        bulk_y.append(to_y(source, new_txt_pieces.at[land], by_send.at[k], by_recv.at[k]))
    bulk_x[0].start()
    bulk_y[0].start()
    bulk_x[1].start()

    scale = jnp.max(jnp.exp(jnp.full((8, 128), scale_ref[0, 0], F32)))
    scale2 = scale * LOG2E
    row_e[...] = jnp.zeros_like(row_e)
    row_m[...] = jnp.zeros_like(row_m)
    col_e[...] = jnp.zeros_like(col_e)
    col_m[...] = jnp.zeros_like(col_m)

    def logit_block(r0, nr, c0, nc, texts, on_rows, kept):
        rows = pl.ds(r0, nr)
        cols = pl.ds(c0, nc)
        dots = lax.dot_general(img[rows, :], texts, (((1,), (1 if on_rows else 0,)), ((), ())), preferred_element_type=F32)
        e = jnp.exp2(dots * scale2)
        if kept:
            exps[pl.ds(r0, kept), cols] = e[:kept]
        m = e * dots
        for values, row_sum, col_sum in ((e, row_e, col_e), (m, row_m, col_m)):
            acc = values[:, 0:128]
            for q in range(1, nc // 128):
                acc = acc + values[:, q * 128:(q + 1) * 128]
            row_sum[rows, :] += acc
            col_sum[:, cols] += jnp.sum(values.reshape(nr // 8, 8, nc), axis=0)

    def own_by_held(slot):
        def body(i, carry):
            part = pl.ds(pl.multiple_of(i * 512, 512), 512)
            logit_block(0, ROWS, pl.multiple_of(slot * ROWS + i * 512, 512), 512, txt[slot, part, :], True, ROWS)
            return carry
        lax.fori_loop(0, 2, body, 0)

    def turn_held(slot):
        def body(i, carry):
            part = pl.ds(pl.multiple_of(i * CHUNK, CHUNK), CHUNK)
            txt_t[:, pl.ds(pl.multiple_of(slot * ROWS + i * CHUNK, CHUNK), CHUNK)] = txt[slot, part, :].T
            return carry
        lax.fori_loop(0, STEPS, body, 0)

    def partner_exps(c0, n):
        dots = lax.dot_general(txt[0], img_p[pl.ds(c0, n), :], (((1,), (1,)), ((), ())), preferred_element_type=F32)
        exps[ROWS:, pl.ds(ROWS + c0, n)] = jnp.exp2(dots * scale2)

    with jax.named_scope("p2"):
        own_by_held(0)
    turn_held(0)

    def diag_body(i, acc):
        part = pl.ds(pl.multiple_of(i * 128, 128), 128)
        prod = img[part, :].astype(F32) * txt[0, part, :].astype(F32)
        return acc + jnp.sum(prod.reshape(16, 8, DIM), axis=0)
    diag_sum = jnp.sum(lax.fori_loop(0, 8, diag_body, jnp.zeros((8, DIM), F32)))

    with jax.named_scope("p3"):
        gather_p.wait_recv()
    with jax.named_scope("p4"):
        own_by_held(1)
    turn_held(1)
    with jax.named_scope("p5"):
        gather_i.wait_recv()
    def partner_own(i, carry):
        with jax.named_scope("p6"):
            partner_exps(pl.multiple_of(i * 512, 512), 512)
        return carry
    with jax.named_scope("p7"):
        lax.fori_loop(0, 2, partner_own, 0)
    for k in range(G_STEPS):
        n_rows = GATHER[k] * PIECE
        done = G_START[k] * PIECE
        new_row = ROWS + done
        with jax.named_scope("p8"):
            gather_x[k].wait_recv()
        relay[k].start()
        if k == 0:
            bulk_y[1].start()
        with jax.named_scope("p9"):
            gather_y[k].wait_recv()
        relay_n[k].start()
        def new_by_held(i, carry, new_row=new_row, n_rows=n_rows):
            c0 = pl.multiple_of(i * 1024, 1024)
            logit_block(new_row, n_rows, c0, 1024, txt_t[:, pl.ds(c0, 1024)], False, 0)
            return carry
        n_held = X_BASE + 2 * done
        logit_block(new_row, n_rows, 0, ROWS, txt_t[:, :ROWS], False, n_rows)
        with jax.named_scope("p10"):
            lax.fori_loop(1, n_held // 1024, new_by_held, 0)
        if n_held % 1024:
            c0 = n_held // 1024 * 1024
            logit_block(new_row, n_rows, c0, n_held - c0, txt_t[:, c0:n_held], False, 0)
        with jax.named_scope("p11"):
            relay[k].wait_recv()
        new_cols = 2 * n_rows
        with jax.named_scope("p12"):
            logit_block(0, new_row + n_rows, n_held, new_cols, far[G_START[k]:G_START[k] + GATHER[k]].reshape(new_cols, DIM), True, ROWS)
        if k + 1 < G_STEPS:
            for p in range(G_START[k], G_START[k] + GATHER[k]):
                c0 = X_BASE + 2 * p * PIECE
                txt_t[:, c0:c0 + 2 * PIECE] = far[p].reshape(2 * PIECE, DIM).T
        if k < 3:
            relay_n[k].wait_recv()
            partner_exps(ROWS + k * CHUNK, CHUNK)

    with jax.named_scope("p13"):
        row_send[...] = jnp.sum(row_e[...].T, axis=0, keepdims=True)
    col_send[...] = jnp.sum(col_e[...], axis=0, keepdims=True)
    swap_row = to_y(row_send, row_recv, row_sem.at[0], row_sem.at[1])
    swap_row.start()
    swap_col = []
    for t, peer in enumerate(peers):
        swap_col.append(to_row(col_send, col_recv.at[t], col_ssem.at[t], col_rsem.at[t], peer))
        swap_col[t].start()
    bulk_x[2].start()
    bulk_y[2].start()
    with jax.named_scope("p14"):
        relay_n[3].wait_recv()
    with jax.named_scope("p15"):
        relay_n[4].wait_recv()
    with jax.named_scope("p16"):
        partner_exps(ROWS + 3 * CHUNK, CHUNK)
    with jax.named_scope("p17"):
        swap_row.wait_recv()
    row_tot = row_send[...] + jnp.concatenate([row_recv[:, ROWS:], row_recv[:, :ROWS]], axis=1)
    row_a = row_e
    row_l[...] = inv_count / row_tot
    swap_a = []
    for t, peer in enumerate(peers):
        swap_a.append(to_row(row_l, all_a.at[t], a_ssem.at[t], a_rsem.at[t], peer))
        swap_a[t].start()
    with jax.named_scope("p18"):
        row_a[...] = jnp.broadcast_to(row_l[...], (128, IMGS)).T
    for t in range(3):
        with jax.named_scope("p19"):
            swap_col[t].wait_recv()
    def slot(ref, s):
        if s < 2:
            return ref[:, s * ROWS:(s + 1) * ROWS]
        starts = [X_BASE + (2 * p + s - 2) * PIECE for p in range(ROWS // PIECE)]
        return jnp.concatenate([ref[:, c:c + PIECE] for c in starts], axis=1)
    for s in range(4):
        tot = (slot(col_send, s) + slot(col_recv.at[0], s ^ 1)) + (slot(col_recv.at[1], s ^ 2) + slot(col_recv.at[2], s ^ 3))
        inverse = inv_count / tot
        if s < 2:
            col_b[:, s * ROWS:(s + 1) * ROWS] = inverse
        else:
            for p in range(ROWS // PIECE):
                start = X_BASE + (2 * p + s - 2) * PIECE
                col_b[:, start:start + PIECE] = inverse[:, p * PIECE:(p + 1) * PIECE]

    def d_img_chunk(r0):
        rows = pl.ds(r0, CHUNK)
        total = None
        for j in range(TXTS // 512):
            g = [exps[rows, c:c + 128] * (row_a[rows, :] + col_b[:, c:c + 128]) for c in range(j * 512, (j + 1) * 512, 128)]
            g = jnp.concatenate([v.astype(BF16) for v in g], axis=1)
            texts = txt[j // 2, j % 2 * 512:(j % 2 + 1) * 512, :] if j < 4 else far[2 * j - 8:2 * j - 6].reshape(512, DIM)
            part = jnp.dot(g, texts, preferred_element_type=F32)
            total = part if total is None else total + part
        return total

    def d_txt_chunk(starts):
        total = None
        for i in range(IMGS // 512):
            rows = slice(i * 512, (i + 1) * 512)
            g = []
            for start in starts:
                cols = pl.ds(start, PIECE)
                g.append((exps[rows, cols] * (row_a[rows, :] + col_b[:, cols])).astype(BF16))
            g = jnp.concatenate(g, axis=1)
            part = lax.dot_general(g, img[rows, :], (((0,), (0,)), ((), ())), preferred_element_type=F32)
            total = part if total is None else total + part
        return total

    swap_b = to_y(col_b, all_b, b_sem.at[0], b_sem.at[1])
    swap_b.start()
    own_r = row_send[:, :ROWS] + row_recv[:, ROWS:]
    loss_part = jnp.sum(jnp.log(own_r) - jnp.log(col_b[:, :ROWS] / inv_count)) - 2.0 * scale * diag_sum
    dscale_part = scale * (jnp.sum(row_a[...] * row_m[...]) + jnp.sum(jnp.sum(col_m[...], axis=0, keepdims=True) * col_b[...])
                           - 2.0 * inv_count * diag_sum)
    lane = lax.broadcasted_iota(jnp.int32, (8, 128), 1)
    scal[0] = jnp.where(lane == 0, loss_part * inv_count, dscale_part)
    send_s = [to_row(scal.at[0], scal.at[t + 1], sc_ssem.at[t], sc_rsem.at[t], peer) for t, peer in enumerate(peers)]
    for t in range(3):
        send_s[t].start()
    for k in range(3, BULK):
        bulk_x[k].start()
        bulk_y[k].start()

    corner = IMGS + ROWS
    d_img_acc = exps.at[pl.ds(ROWS, ROWS), pl.ds(corner, DIM)]
    d_txt_acc = exps.at[pl.ds(ROWS, ROWS), pl.ds(corner + DIM, DIM)]

    def fix_body(i, carry):
        part = pl.ds(pl.multiple_of(i * 128, 128), 128)
        on_diag = lax.broadcasted_iota(jnp.int32, (128, 128), 0) == lax.broadcasted_iota(jnp.int32, (128, 128), 1)
        term = (2.0 * inv_count) / (row_a[part, :] + col_b[:, part])
        exps[part, part] = exps[part, part] - jnp.where(on_diag, term, 0.0)
        return carry
    lax.fori_loop(0, ROWS // 128, fix_body, 0)
    txt_b[...] = jnp.broadcast_to(col_b[:, :ROWS], (128, ROWS)).T

    def tile_body(k, carry):
        first = pl.multiple_of(k * CHUNK, CHUNK)
        part = pl.ds(first, CHUNK)
        d_img_acc[part, :] = d_img_chunk(first)
        d_txt_acc[part, :] = d_txt_chunk((first, first + PIECE))
        return carry
    with jax.named_scope("p20"):
        lax.fori_loop(0, STEPS, tile_body, 0)

    for t in range(3):
        with jax.named_scope("p21"):
            swap_a[t].wait_recv()
        with jax.named_scope("p22"):
            send_s[t].wait_recv()
    with jax.named_scope("p23"):
        swap_b.wait_recv()
    direct_b = jnp.concatenate([slot(all_b, 0), slot(all_b, 2)], axis=1)
    relayed_b = jnp.concatenate([slot(all_b, 1), slot(all_b, 3)], axis=1)
    for k in range(BULK):
        src_a, dst, size = (PIECE * v for v in bulk_span(k))
        src_b = PIECE * TXT_START[k]
        for to, direct, relayed, src in ((new_a, all_a[1], all_a[2], src_a), (new_b, direct_b, relayed_b, src_b)):
            to[:, dst:dst + size] = direct[:, src:src + size]
            to[:, dst + size:dst + 2 * size] = relayed[:, src:src + size]
    scal_y[0] = (scal[0] + scal[1]) + (scal[2] + scal[3])
    swap_s = to_y(scal_y.at[0], scal_y.at[1], sc_ssem.at[3], sc_rsem.at[3])
    swap_s.start()

    def partner_body(k, carry):
        first = pl.multiple_of(k * CHUNK, CHUNK)
        part = pl.ds(first, CHUNK)
        low = pl.ds(ROWS + first, CHUNK)
        total = None
        for j in range(IMGS // 512):
            g = [exps[low, ROWS + c:ROWS + c + 128] * (txt_b[part, :] + all_a[0, :, c:c + 128]) for c in range(j * 512, (j + 1) * 512, 128)]
            g = jnp.concatenate([v.astype(BF16) for v in g], axis=1)
            more = jnp.dot(g, img_p[j * 512:(j + 1) * 512, :], preferred_element_type=F32)
            total = more if total is None else total + more
        d_txt_acc[part, :] += total
        return carry

    def outside(own, own_factor, others, factor, total):
        dots = lax.dot_general(own, others, (((1,), (1,)), ((), ())), preferred_element_type=F32)
        e = jnp.exp2(dots * scale2)
        g = [(e[:, c:c + 128] * (own_factor + factor[:, c:c + 128])).astype(BF16) for c in range(0, others.shape[0], 128)]
        total[...] += jnp.dot(jnp.concatenate(g, axis=1), others, preferred_element_type=F32)

    def both_sides(start, size):
        part = pl.ds(start, size)
        outside(txt[0], txt_b[...], new_img[part, :], new_a[:, part], d_txt_acc)
        outside(img[0:ROWS, :], row_a[0:ROWS, :], new_txt[part, :], new_b[:, part], d_img_acc)

    def relays(k, dst, size):
        direct, relayed = pl.ds(dst, size), pl.ds(dst + size, size)
        rx = to_row(new_img_pieces.at[direct], new_img_pieces.at[relayed], fx_send.at[k], fx_recv.at[k], partner)
        ry = to_row(new_txt_pieces.at[direct], new_txt_pieces.at[relayed], fy_send.at[k], fy_recv.at[k], partner)
        return rx, ry

    def land(k, dst, size):
        direct = pl.ds(dst, size)
        rx, ry = relays(k, dst, size)
        to_row(new_img_pieces.at[direct], new_img_pieces.at[direct], bx_send.at[k], bx_recv.at[k], across).wait_recv()
        rx.start()
        to_y(new_txt_pieces.at[direct], new_txt_pieces.at[direct], by_send.at[k], by_recv.at[k]).wait_recv()
        ry.start()

    def relayed_in(k, dst, size):
        for copy in relays(k, dst, size):
            copy.wait_recv()

    def sent(k, dst, size):
        direct = pl.ds(dst, size)
        to_row(new_img_pieces.at[direct], new_img_pieces.at[direct], bx_send.at[k], bx_recv.at[k], across).wait_send()
        to_y(new_txt_pieces.at[direct], new_txt_pieces.at[direct], by_send.at[k], by_recv.at[k]).wait_send()
        for copy in relays(k, dst, size):
            copy.wait_send()

    def early_sent():
        for k in range(G_STEPS):
            gather_x[k].wait_send()
            gather_y[k].wait_send()
            relay[k].wait_send()
            relay_n[k].wait_send()
        for k in range(2):
            sent(k, *bulk_span(k)[1:])
        gather_p.wait_send()
        gather_i.wait_send()
        swap_b.wait_send()
        swap_row.wait_send()
        for t in range(3):
            swap_col[t].wait_send()
            send_s[t].wait_send()
            swap_a[t].wait_send()

    for k in range(3):
        with jax.named_scope("p24"):
            land(k, *bulk_span(k)[1:])
    with jax.named_scope("p25"):
        lax.fori_loop(0, STEPS, partner_body, 0)
    for k in range(2):
        with jax.named_scope("p26"):
            relayed_in(k, *bulk_span(k)[1:])

    def bulk_body(k, carry):
        @pl.when(k == 5)
        def _():
            early_sent()
        @pl.when(k >= 3)
        def _():
            land(k, 4 * k - 2, 2)
            relayed_in(k - 1, 4 * k - 6, 2)
            sent(k - 1, 4 * k - 6, 2)
        with jax.named_scope("p27"):
            both_sides(pl.multiple_of(2 * (k - 1) * CHUNK, CHUNK), 2 * CHUNK)
        return carry
    lax.fori_loop(1, BULK - 1, bulk_body, 0)

    src, dst, size = bulk_span(BULK - 1)
    with jax.named_scope("p28"):
        land(BULK - 1, dst, size)
    with jax.named_scope("p29"):
        relayed_in(BULK - 2, dst - 4, 2)
    with jax.named_scope("p30"):
        both_sides(dst * PIECE - CHUNK, CHUNK + PIECE)
    with jax.named_scope("p31"):
        relayed_in(BULK - 1, dst, size)
    with jax.named_scope("p32"):
        both_sides((dst + 1) * PIECE, PIECE)

    with jax.named_scope("p33"):
        dimg_ref[...] = (scale * d_img_acc[...]).astype(BF16)
    dtxt_ref[...] = (scale * d_txt_acc[...]).astype(BF16)

    with jax.named_scope("p34"):
        swap_s.wait_recv()
    total = scal_y[0] + scal_y[1]
    loss_ref[0, 0] = total[0, 0]
    dscale_ref[0, 0] = total[0, 1]

    for k in range(BULK - 2, BULK):
        with jax.named_scope("p35"):
            sent(k, *bulk_span(k)[1:])
    swap_s.wait_send()


def put_kernel(img_in, txt_in, img_out, txt_out, sems):
    copies = [pltpu.make_async_copy(img_in, img_out, sems.at[0]), pltpu.make_async_copy(txt_in, txt_out, sems.at[1])]
    for copy in copies:
        copy.start()
    for copy in copies:
        copy.wait()


def solution(mesh):
    batch_spec = P(("row", "col"), None)
    n_dev = mesh.shape["row"] * mesh.shape["col"]
    inv_count = 1.0 / (2 * ROWS * n_dev)
    dma = pltpu.SemaphoreType.DMA

    def local_tile(img_loc, txt_loc, log_scale):
        any_spec = pl.BlockSpec(memory_space=pl.ANY)
        vmem_spec = pl.BlockSpec(memory_space=pltpu.VMEM)
        smem_spec = pl.BlockSpec(memory_space=pltpu.SMEM)
        loss, d_img, d_txt, d_scale = pl.pallas_call(
            functools.partial(kernel, inv_count),
            out_shape=(
                jax.ShapeDtypeStruct((1, 1), F32),
                pltpu.VMEM((ROWS, DIM), BF16),
                pltpu.VMEM((ROWS, DIM), BF16),
                jax.ShapeDtypeStruct((1, 1), F32),
            ),
            in_specs=[smem_spec, any_spec, any_spec],
            out_specs=(smem_spec, vmem_spec, vmem_spec, smem_spec),
            scratch_shapes=[
                pltpu.VMEM((IMGS, DIM), BF16),
                pltpu.VMEM((2, ROWS, DIM), BF16),
                pltpu.VMEM((ROWS // PIECE, 2, PIECE, DIM), BF16),
                pltpu.VMEM((DIM, TXTS), BF16),
                pltpu.VMEM((IMGS, DIM), BF16),
                pltpu.VMEM((TXTS, DIM), BF16),
                pltpu.VMEM((TXTS, DIM), BF16),
                pltpu.VMEM((IMGS, TXTS), F32),
                pltpu.VMEM((IMGS, 128), F32),
                pltpu.VMEM((IMGS, 128), F32),
                pltpu.VMEM((8, TXTS), F32),
                pltpu.VMEM((8, TXTS), F32),
                pltpu.VMEM((1, IMGS), F32),
                pltpu.VMEM((1, IMGS), F32),
                pltpu.VMEM((1, TXTS), F32),
                pltpu.VMEM((3, 1, TXTS), F32),
                pltpu.VMEM((1, TXTS), F32),
                pltpu.VMEM((1, IMGS), F32),
                pltpu.VMEM((3, 1, IMGS), F32),
                pltpu.VMEM((1, TXTS), F32),
                pltpu.VMEM((1, TXTS), F32),
                pltpu.VMEM((1, TXTS), F32),
                pltpu.VMEM((ROWS, 128), F32),
                pltpu.VMEM((4, 8, 128), F32),
                pltpu.VMEM((2, 8, 128), F32),
                dma((2 * G_STEPS,)),
                dma((G_STEPS,)), dma((G_STEPS,)),
                dma((G_STEPS,)), dma((G_STEPS,)),
                dma((4,)),
                dma((G_STEPS,)), dma((G_STEPS,)),
                dma((2,)),
                dma((3,)), dma((3,)),
                dma((BULK,)), dma((BULK,)), dma((BULK,)), dma((BULK,)),
                dma((BULK,)), dma((BULK,)), dma((BULK,)), dma((BULK,)),
                dma((G_STEPS,)), dma((G_STEPS,)),
                dma((3,)), dma((3,)), dma((2,)),
                dma((4,)), dma((4,)),
            ],
            compiler_params=pltpu.CompilerParams(
                collective_id=0, has_side_effects=True, vmem_limit_bytes=VMEM_LIMIT,
            ),
            name="clip_loss",
        )(log_scale.reshape(1, 1), img_loc, txt_loc)
        rows_shape = jax.ShapeDtypeStruct((ROWS, DIM), BF16)
        d_img, d_txt = pl.pallas_call(
            put_kernel,
            out_shape=(rows_shape, rows_shape),
            in_specs=[vmem_spec, vmem_spec],
            out_specs=(any_spec, any_spec),
            scratch_shapes=[dma((2,))],
            compiler_params=pltpu.CompilerParams(vmem_limit_bytes=MARGIN),
            name="put_rows",
        )(d_img, d_txt)
        return loss.reshape(()), d_img, d_txt, d_scale.reshape(())

    return jax.shard_map(local_tile, mesh=mesh, in_specs=(batch_spec, batch_spec, P()), out_specs=(P(), batch_spec, batch_spec, P()), check_vma=False)
```

```python
import functools
import math

import jax
import jax.numpy as jnp
from jax import lax
from jax.experimental import pallas as pl
from jax.experimental.pallas import tpu as pltpu
from jax.sharding import PartitionSpec as P

MESH = pl.DeviceIdType.MESH
VMEM_LIMIT = 247 * 256 * 1024
MARGIN = 4 * 1024 * 1024
F32 = jnp.float32
BF16 = jnp.bfloat16
ROWS = 1024
DIM = 512
CHUNK = 256
STEPS = ROWS // CHUNK
SIZES = (2, 1, 2, 2, 2, 2, 2, 2, 1)
TXT_START = (0, 8, 2, 4, 6, 9, 11, 13, 15)
BULK = len(SIZES)
PIECE = 128
GATHER = (2, 2, 2, 1, 1)
G_START = tuple(sum(GATHER[:k]) for k in range(len(GATHER)))
G_STEPS = len(GATHER)
IMGS = 2 * ROWS
TXTS = 4 * ROWS
X_BASE = 2 * ROWS
LOG2E = math.log2(math.e)


def kernel(inv_count, scale_ref, img_hbm, txt_hbm, scal_ref, dimg_ref, dtxt_ref,
           img, txt, far, txt_t, img_p, new_txt, new_img, exps, row_e, row_m, col_e, col_m, row_send, row_recv, col_send, col_recv, col_b, row_l, all_a, all_b, new_a, new_b, txt_b,
           scal, scal_y, load_sem, gy_send, gy_recv, gx_send, gx_recv, gp_sem, gf_send, gf_recv, row_sem, col_ssem, col_rsem,
           bx_send, bx_recv, by_send, by_recv, fx_send, fx_recv, fy_send, fy_recv, pn_send, pn_recv,
           a_ssem, a_rsem, b_sem, sc_ssem, sc_rsem):
    row = lax.axis_index("row")
    col = lax.axis_index("col")
    core = lax.rem(row, 2)
    partner = row + 1 - 2 * core
    across = lax.rem(row + 2, 4)
    diagonal = across + 1 - 2 * core
    peers = (partner, across, diagonal)
    other_col = 1 - col

    def to_y(src, dst, ssem, rsem):
        return pltpu.make_async_remote_copy(src, dst, ssem, rsem, device_id={"row": row, "col": other_col}, device_id_type=MESH)

    def to_row(src, dst, ssem, rsem, peer):
        return pltpu.make_async_remote_copy(src, dst, ssem, rsem, device_id={"row": peer, "col": col}, device_id_type=MESH)

    txt_pieces = txt.at[0].reshape(ROWS // PIECE, PIECE, DIM)
    loads = []
    for k in range(G_STEPS):
        part = pl.ds(G_START[k] * PIECE, GATHER[k] * PIECE)
        loads.append((pltpu.make_async_copy(txt_hbm.at[part], txt.at[0, part], load_sem.at[k]),
                      pltpu.make_async_copy(img_hbm.at[part], img.at[part], load_sem.at[G_STEPS + k])))
        for copy in loads[k]:
            copy.start()

    barrier = pltpu.get_barrier_semaphore()
    for peer in peers:
        pl.semaphore_signal(barrier, inc=1, device_id={"row": peer, "col": col}, device_id_type=MESH)
    pl.semaphore_signal(barrier, inc=1, device_id={"row": row, "col": other_col}, device_id_type=MESH)

    pl.semaphore_wait(barrier, 4)

    gather_y, gather_x, relay = [], [], []
    for k in range(G_STEPS):
        pieces = pl.ds(G_START[k], GATHER[k])
        part = pl.ds(G_START[k] * PIECE, GATHER[k] * PIECE)
        gather_x.append(to_row(txt_pieces.at[pieces], far.at[pieces, 0], gx_send.at[k], gx_recv.at[k], across))
        gather_y.append(to_y(img.at[part], img.at[pl.ds(ROWS + G_START[k] * PIECE, GATHER[k] * PIECE)], gy_send.at[k], gy_recv.at[k]))
        relay.append(to_row(far.at[pieces, 0], far.at[pieces, 1], gf_send.at[k], gf_recv.at[k], partner))
        loads[k][0].wait()
        gather_x[k].start()
        loads[k][1].wait()
        gather_y[k].start()
    gather_p = to_row(txt.at[0], txt.at[1], gp_sem.at[0], gp_sem.at[1], partner)
    gather_p.start()
    gather_i = to_row(img.at[pl.ds(0, ROWS)], img_p.at[pl.ds(0, ROWS)], gp_sem.at[2], gp_sem.at[3], partner)
    gather_i.start()
    relay_n = []
    for k in range(G_STEPS):
        part = pl.ds(ROWS + G_START[k] * PIECE, GATHER[k] * PIECE)
        relay_n.append(to_row(img.at[part], img_p.at[part], pn_send.at[k], pn_recv.at[k], partner))

    img_pieces = img.reshape(IMGS // PIECE, PIECE, DIM)
    new_img_pieces = new_img.reshape(TXTS // PIECE, PIECE, DIM)
    new_txt_pieces = new_txt.reshape(TXTS // PIECE, PIECE, DIM)

    def bulk_span(k):
        start = sum(SIZES[:k])
        return start, 2 * start, SIZES[k]

    bulk_x, bulk_y = [], []
    for k in range(BULK):
        src, dst, size = bulk_span(k)
        land = pl.ds(dst, size)
        bulk_x.append(to_row(img_pieces.at[pl.ds(src, size)], new_img_pieces.at[land], bx_send.at[k], bx_recv.at[k], across))
        half = ROWS // PIECE
        src = TXT_START[k]
        source = txt_pieces.at[pl.ds(src, size)] if src < half else far.at[pl.ds(src - half, size), 0]
        bulk_y.append(to_y(source, new_txt_pieces.at[land], by_send.at[k], by_recv.at[k]))
    bulk_x[0].start()
    bulk_y[0].start()
    bulk_x[1].start()

    scale = jnp.max(jnp.exp(jnp.full((8, 128), scale_ref[0, 0], F32)))
    scale2 = scale * LOG2E
    row_e[...] = jnp.zeros_like(row_e)
    row_m[...] = jnp.zeros_like(row_m)
    col_e[...] = jnp.zeros_like(col_e)
    col_m[...] = jnp.zeros_like(col_m)

    def logit_block(r0, nr, c0, nc, texts, on_rows, kept):
        rows = pl.ds(r0, nr)
        cols = pl.ds(c0, nc)
        dots = lax.dot_general(img[rows, :], texts, (((1,), (1 if on_rows else 0,)), ((), ())), preferred_element_type=F32)
        e = jnp.exp2(dots * scale2)
        if kept:
            exps[pl.ds(r0, kept), cols] = e[:kept]
        m = e * dots
        for values, row_sum, col_sum in ((e, row_e, col_e), (m, row_m, col_m)):
            acc = values[:, 0:128]
            for q in range(1, nc // 128):
                acc = acc + values[:, q * 128:(q + 1) * 128]
            row_sum[rows, :] += acc
            col_sum[:, cols] += jnp.sum(values.reshape(nr // 8, 8, nc), axis=0)

    def own_by_held(slot):
        def body(i, carry):
            part = pl.ds(pl.multiple_of(i * 512, 512), 512)
            logit_block(0, ROWS, pl.multiple_of(slot * ROWS + i * 512, 512), 512, txt[slot, part, :], True, ROWS)
            return carry
        lax.fori_loop(0, 2, body, 0)

    def turn_held(slot):
        def body(i, carry):
            part = pl.ds(pl.multiple_of(i * CHUNK, CHUNK), CHUNK)
            txt_t[:, pl.ds(pl.multiple_of(slot * ROWS + i * CHUNK, CHUNK), CHUNK)] = txt[slot, part, :].T
            return carry
        lax.fori_loop(0, STEPS, body, 0)

    def partner_exps(c0, n):
        dots = lax.dot_general(txt[0], img_p[pl.ds(c0, n), :], (((1,), (1,)), ((), ())), preferred_element_type=F32)
        exps[ROWS:, pl.ds(ROWS + c0, n)] = jnp.exp2(dots * scale2)

    own_by_held(0)
    turn_held(0)

    def diag_body(i, acc):
        part = pl.ds(pl.multiple_of(i * 128, 128), 128)
        prod = img[part, :].astype(F32) * txt[0, part, :].astype(F32)
        return acc + jnp.sum(prod.reshape(16, 8, DIM), axis=0)
    diag_sum = jnp.sum(lax.fori_loop(0, 8, diag_body, jnp.zeros((8, DIM), F32)))

    gather_p.wait_recv()
    own_by_held(1)
    turn_held(1)
    gather_i.wait_recv()
    def partner_own(i, carry):
        partner_exps(pl.multiple_of(i * 512, 512), 512)
        return carry
    lax.fori_loop(0, 2, partner_own, 0)
    for k in range(G_STEPS):
        n_rows = GATHER[k] * PIECE
        done = G_START[k] * PIECE
        new_row = ROWS + done
        gather_x[k].wait_recv()
        relay[k].start()
        if k == 0:
            bulk_y[1].start()
        gather_y[k].wait_recv()
        relay_n[k].start()
        def new_by_held(i, carry, new_row=new_row, n_rows=n_rows):
            c0 = pl.multiple_of(i * 1024, 1024)
            logit_block(new_row, n_rows, c0, 1024, txt_t[:, pl.ds(c0, 1024)], False, 0)
            return carry
        n_held = X_BASE + 2 * done
        logit_block(new_row, n_rows, 0, ROWS, txt_t[:, :ROWS], False, n_rows)
        lax.fori_loop(1, n_held // 1024, new_by_held, 0)
        if n_held % 1024:
            c0 = n_held // 1024 * 1024
            logit_block(new_row, n_rows, c0, n_held - c0, txt_t[:, c0:n_held], False, 0)
        relay[k].wait_recv()
        new_cols = 2 * n_rows
        logit_block(0, new_row + n_rows, n_held, new_cols, far[G_START[k]:G_START[k] + GATHER[k]].reshape(new_cols, DIM), True, ROWS)
        if k + 1 < G_STEPS:
            for p in range(G_START[k], G_START[k] + GATHER[k]):
                c0 = X_BASE + 2 * p * PIECE
                txt_t[:, c0:c0 + 2 * PIECE] = far[p].reshape(2 * PIECE, DIM).T
        if k < 3:
            relay_n[k].wait_recv()
            partner_exps(ROWS + k * CHUNK, CHUNK)

    row_send[...] = jnp.sum(row_e[...].T, axis=0, keepdims=True)
    col_send[...] = jnp.sum(col_e[...], axis=0, keepdims=True)
    swap_row = to_y(row_send, row_recv, row_sem.at[0], row_sem.at[1])
    swap_row.start()
    swap_col = []
    for t, peer in enumerate(peers):
        swap_col.append(to_row(col_send, col_recv.at[t], col_ssem.at[t], col_rsem.at[t], peer))
        swap_col[t].start()
    bulk_x[2].start()
    bulk_y[2].start()
    relay_n[3].wait_recv()
    relay_n[4].wait_recv()
    partner_exps(ROWS + 3 * CHUNK, CHUNK)
    swap_row.wait_recv()
    row_tot = row_send[...] + jnp.concatenate([row_recv[:, ROWS:], row_recv[:, :ROWS]], axis=1)
    row_a = row_e
    row_l[...] = inv_count / row_tot
    swap_a = []
    for t, peer in enumerate(peers):
        swap_a.append(to_row(row_l, all_a.at[t], a_ssem.at[t], a_rsem.at[t], peer))
        swap_a[t].start()
    row_a[...] = jnp.broadcast_to(row_l[...], (128, IMGS)).T
    for t in range(3):
        swap_col[t].wait_recv()
    def slot(ref, s):
        if s < 2:
            return ref[:, s * ROWS:(s + 1) * ROWS]
        starts = [X_BASE + (2 * p + s - 2) * PIECE for p in range(ROWS // PIECE)]
        return jnp.concatenate([ref[:, c:c + PIECE] for c in starts], axis=1)
    for s in range(4):
        tot = (slot(col_send, s) + slot(col_recv.at[0], s ^ 1)) + (slot(col_recv.at[1], s ^ 2) + slot(col_recv.at[2], s ^ 3))
        inverse = inv_count / tot
        if s < 2:
            col_b[:, s * ROWS:(s + 1) * ROWS] = inverse
        else:
            for p in range(ROWS // PIECE):
                start = X_BASE + (2 * p + s - 2) * PIECE
                col_b[:, start:start + PIECE] = inverse[:, p * PIECE:(p + 1) * PIECE]

    def d_img_chunk(r0):
        rows = pl.ds(r0, CHUNK)
        total = None
        for j in range(TXTS // 512):
            g = [exps[rows, c:c + 128] * (row_a[rows, :] + col_b[:, c:c + 128]) for c in range(j * 512, (j + 1) * 512, 128)]
            g = jnp.concatenate([v.astype(BF16) for v in g], axis=1)
            texts = txt[j // 2, j % 2 * 512:(j % 2 + 1) * 512, :] if j < 4 else far[2 * j - 8:2 * j - 6].reshape(512, DIM)
            part = jnp.dot(g, texts, preferred_element_type=F32)
            total = part if total is None else total + part
        return total

    def d_txt_chunk(starts):
        total = None
        for i in range(IMGS // 512):
            rows = slice(i * 512, (i + 1) * 512)
            g = []
            for start in starts:
                cols = pl.ds(start, PIECE)
                g.append((exps[rows, cols] * (row_a[rows, :] + col_b[:, cols])).astype(BF16))
            g = jnp.concatenate(g, axis=1)
            part = lax.dot_general(g, img[rows, :], (((0,), (0,)), ((), ())), preferred_element_type=F32)
            total = part if total is None else total + part
        return total

    swap_b = to_y(col_b, all_b, b_sem.at[0], b_sem.at[1])
    swap_b.start()
    own_r = row_send[:, :ROWS] + row_recv[:, ROWS:]
    loss_part = jnp.sum(jnp.log(own_r) - jnp.log(col_b[:, :ROWS] / inv_count)) - 2.0 * scale * diag_sum
    dscale_part = scale * (jnp.sum(row_a[...] * row_m[...]) + jnp.sum(jnp.sum(col_m[...], axis=0, keepdims=True) * col_b[...])
                           - 2.0 * inv_count * diag_sum)
    lane = lax.broadcasted_iota(jnp.int32, (8, 128), 1)
    scal[0] = jnp.where(lane == 0, loss_part * inv_count, dscale_part)
    send_s = [to_row(scal.at[0], scal.at[t + 1], sc_ssem.at[t], sc_rsem.at[t], peer) for t, peer in enumerate(peers)]
    for t in range(3):
        send_s[t].start()
    for k in range(3, BULK):
        bulk_x[k].start()
        bulk_y[k].start()

    corner = IMGS + ROWS
    d_img_acc = exps.at[pl.ds(ROWS, ROWS), pl.ds(corner, DIM)]
    d_txt_acc = exps.at[pl.ds(ROWS, ROWS), pl.ds(corner + DIM, DIM)]

    def fix_body(i, carry):
        part = pl.ds(pl.multiple_of(i * 128, 128), 128)
        on_diag = lax.broadcasted_iota(jnp.int32, (128, 128), 0) == lax.broadcasted_iota(jnp.int32, (128, 128), 1)
        term = (2.0 * inv_count) / (row_a[part, :] + col_b[:, part])
        exps[part, part] = exps[part, part] - jnp.where(on_diag, term, 0.0)
        return carry
    lax.fori_loop(0, ROWS // 128, fix_body, 0)
    txt_b[...] = jnp.broadcast_to(col_b[:, :ROWS], (128, ROWS)).T

    def tile_body(k, carry):
        first = pl.multiple_of(k * CHUNK, CHUNK)
        part = pl.ds(first, CHUNK)
        d_img_acc[part, :] = d_img_chunk(first)
        d_txt_acc[part, :] = d_txt_chunk((first, first + PIECE))
        return carry
    lax.fori_loop(0, STEPS, tile_body, 0)

    for t in range(3):
        swap_a[t].wait_recv()
        send_s[t].wait_recv()
    swap_b.wait_recv()
    direct_b = jnp.concatenate([slot(all_b, 0), slot(all_b, 2)], axis=1)
    relayed_b = jnp.concatenate([slot(all_b, 1), slot(all_b, 3)], axis=1)
    for k in range(BULK):
        src_a, dst, size = (PIECE * v for v in bulk_span(k))
        src_b = PIECE * TXT_START[k]
        for to, direct, relayed, src in ((new_a, all_a[1], all_a[2], src_a), (new_b, direct_b, relayed_b, src_b)):
            to[:, dst:dst + size] = direct[:, src:src + size]
            to[:, dst + size:dst + 2 * size] = relayed[:, src:src + size]
    scal_y[0] = (scal[0] + scal[1]) + (scal[2] + scal[3])
    swap_s = to_y(scal_y.at[0], scal_y.at[1], sc_ssem.at[3], sc_rsem.at[3])
    swap_s.start()

    def partner_body(k, carry):
        first = pl.multiple_of(k * CHUNK, CHUNK)
        part = pl.ds(first, CHUNK)
        low = pl.ds(ROWS + first, CHUNK)
        total = None
        for j in range(IMGS // 512):
            g = [exps[low, ROWS + c:ROWS + c + 128] * (txt_b[part, :] + all_a[0, :, c:c + 128]) for c in range(j * 512, (j + 1) * 512, 128)]
            g = jnp.concatenate([v.astype(BF16) for v in g], axis=1)
            more = jnp.dot(g, img_p[j * 512:(j + 1) * 512, :], preferred_element_type=F32)
            total = more if total is None else total + more
        d_txt_acc[part, :] += total
        return carry

    def outside(own, own_factor, others, factor, total):
        dots = lax.dot_general(own, others, (((1,), (1,)), ((), ())), preferred_element_type=F32)
        e = jnp.exp2(dots * scale2)
        g = [(e[:, c:c + 128] * (own_factor + factor[:, c:c + 128])).astype(BF16) for c in range(0, others.shape[0], 128)]
        total[...] += jnp.dot(jnp.concatenate(g, axis=1), others, preferred_element_type=F32)

    def both_sides(start, size):
        part = pl.ds(start, size)
        outside(txt[0], txt_b[...], new_img[part, :], new_a[:, part], d_txt_acc)
        outside(img[0:ROWS, :], row_a[0:ROWS, :], new_txt[part, :], new_b[:, part], d_img_acc)

    def relays(k, dst, size):
        direct, relayed = pl.ds(dst, size), pl.ds(dst + size, size)
        rx = to_row(new_img_pieces.at[direct], new_img_pieces.at[relayed], fx_send.at[k], fx_recv.at[k], partner)
        ry = to_row(new_txt_pieces.at[direct], new_txt_pieces.at[relayed], fy_send.at[k], fy_recv.at[k], partner)
        return rx, ry

    def land(k, dst, size):
        direct = pl.ds(dst, size)
        rx, ry = relays(k, dst, size)
        to_row(new_img_pieces.at[direct], new_img_pieces.at[direct], bx_send.at[k], bx_recv.at[k], across).wait_recv()
        rx.start()
        to_y(new_txt_pieces.at[direct], new_txt_pieces.at[direct], by_send.at[k], by_recv.at[k]).wait_recv()
        ry.start()

    def relayed_in(k, dst, size):
        for copy in relays(k, dst, size):
            copy.wait_recv()

    def sent(k, dst, size):
        direct = pl.ds(dst, size)
        to_row(new_img_pieces.at[direct], new_img_pieces.at[direct], bx_send.at[k], bx_recv.at[k], across).wait_send()
        to_y(new_txt_pieces.at[direct], new_txt_pieces.at[direct], by_send.at[k], by_recv.at[k]).wait_send()
        for copy in relays(k, dst, size):
            copy.wait_send()

    def early_sent():
        for k in range(G_STEPS):
            gather_x[k].wait_send()
            gather_y[k].wait_send()
            relay[k].wait_send()
            relay_n[k].wait_send()
        for k in range(2):
            sent(k, *bulk_span(k)[1:])
        gather_p.wait_send()
        gather_i.wait_send()
        swap_b.wait_send()
        swap_row.wait_send()
        for t in range(3):
            swap_col[t].wait_send()
            send_s[t].wait_send()
            swap_a[t].wait_send()

    for k in range(3):
        land(k, *bulk_span(k)[1:])
    lax.fori_loop(0, STEPS, partner_body, 0)
    for k in range(2):
        relayed_in(k, *bulk_span(k)[1:])

    def bulk_body(k, carry):
        @pl.when(k == 5)
        def _():
            early_sent()
        @pl.when(k >= 3)
        def _():
            land(k, 4 * k - 2, 2)
            relayed_in(k - 1, 4 * k - 6, 2)
            sent(k - 1, 4 * k - 6, 2)
        both_sides(pl.multiple_of(2 * (k - 1) * CHUNK, CHUNK), 2 * CHUNK)
        return carry
    lax.fori_loop(1, BULK - 1, bulk_body, 0)

    src, dst, size = bulk_span(BULK - 1)
    land(BULK - 1, dst, size)
    relayed_in(BULK - 2, dst - 4, 2)
    both_sides(dst * PIECE - CHUNK, CHUNK + PIECE)
    relayed_in(BULK - 1, dst, size)
    both_sides((dst + 1) * PIECE, PIECE)

    dimg_ref[...] = (scale * d_img_acc[...]).astype(BF16)
    dtxt_ref[...] = (scale * d_txt_acc[...]).astype(BF16)

    swap_s.wait_recv()
    scal_ref[...] = scal_y[0] + scal_y[1]

    for k in range(BULK - 2, BULK):
        sent(k, *bulk_span(k)[1:])
    swap_s.wait_send()


def put_kernel(scal_in, img_in, txt_in, loss_out, img_out, txt_out, dscale_out, loss_cell, dscale_cell, sems):
    copies = [pltpu.make_async_copy(img_in, img_out, sems.at[0]), pltpu.make_async_copy(txt_in, txt_out, sems.at[1])]
    for copy in copies:
        copy.start()
    loss_cell[0, 0] = scal_in[0, 0]
    dscale_cell[0, 0] = scal_in[0, 1]
    cells = [pltpu.make_async_copy(loss_cell, loss_out, sems.at[2]), pltpu.make_async_copy(dscale_cell, dscale_out, sems.at[3])]
    for copy in cells:
        copy.start()
    for copy in copies + cells:
        copy.wait()


def solution(mesh):
    batch_spec = P(("row", "col"), None)
    n_dev = mesh.shape["row"] * mesh.shape["col"]
    inv_count = 1.0 / (2 * ROWS * n_dev)
    dma = pltpu.SemaphoreType.DMA

    def local_tile(img_loc, txt_loc, log_scale):
        any_spec = pl.BlockSpec(memory_space=pl.ANY)
        vmem_spec = pl.BlockSpec(memory_space=pltpu.VMEM)
        smem_spec = pl.BlockSpec(memory_space=pltpu.SMEM)
        scalars, d_img, d_txt = pl.pallas_call(
            functools.partial(kernel, inv_count),
            out_shape=(
                pltpu.VMEM((8, 128), F32),
                pltpu.VMEM((ROWS, DIM), BF16),
                pltpu.VMEM((ROWS, DIM), BF16),
            ),
            in_specs=[smem_spec, any_spec, any_spec],
            out_specs=(vmem_spec, vmem_spec, vmem_spec),
            scratch_shapes=[
                pltpu.VMEM((IMGS, DIM), BF16),
                pltpu.VMEM((2, ROWS, DIM), BF16),
                pltpu.VMEM((ROWS // PIECE, 2, PIECE, DIM), BF16),
                pltpu.VMEM((DIM, TXTS), BF16),
                pltpu.VMEM((IMGS, DIM), BF16),
                pltpu.VMEM((TXTS, DIM), BF16),
                pltpu.VMEM((TXTS, DIM), BF16),
                pltpu.VMEM((IMGS, TXTS), F32),
                pltpu.VMEM((IMGS, 128), F32),
                pltpu.VMEM((IMGS, 128), F32),
                pltpu.VMEM((8, TXTS), F32),
                pltpu.VMEM((8, TXTS), F32),
                pltpu.VMEM((1, IMGS), F32),
                pltpu.VMEM((1, IMGS), F32),
                pltpu.VMEM((1, TXTS), F32),
                pltpu.VMEM((3, 1, TXTS), F32),
                pltpu.VMEM((1, TXTS), F32),
                pltpu.VMEM((1, IMGS), F32),
                pltpu.VMEM((3, 1, IMGS), F32),
                pltpu.VMEM((1, TXTS), F32),
                pltpu.VMEM((1, TXTS), F32),
                pltpu.VMEM((1, TXTS), F32),
                pltpu.VMEM((ROWS, 128), F32),
                pltpu.VMEM((4, 8, 128), F32),
                pltpu.VMEM((2, 8, 128), F32),
                dma((2 * G_STEPS,)),
                dma((G_STEPS,)), dma((G_STEPS,)),
                dma((G_STEPS,)), dma((G_STEPS,)),
                dma((4,)),
                dma((G_STEPS,)), dma((G_STEPS,)),
                dma((2,)),
                dma((3,)), dma((3,)),
                dma((BULK,)), dma((BULK,)), dma((BULK,)), dma((BULK,)),
                dma((BULK,)), dma((BULK,)), dma((BULK,)), dma((BULK,)),
                dma((G_STEPS,)), dma((G_STEPS,)),
                dma((3,)), dma((3,)), dma((2,)),
                dma((4,)), dma((4,)),
            ],
            compiler_params=pltpu.CompilerParams(
                collective_id=0, has_side_effects=True, vmem_limit_bytes=VMEM_LIMIT,
            ),
            name="clip_loss",
        )(log_scale.reshape(1, 1), img_loc, txt_loc)
        rows_shape = jax.ShapeDtypeStruct((ROWS, DIM), BF16)
        cell_shape = jax.ShapeDtypeStruct((1, 1), F32)
        loss, d_img, d_txt, d_scale = pl.pallas_call(
            put_kernel,
            out_shape=(cell_shape, rows_shape, rows_shape, cell_shape),
            in_specs=[vmem_spec, vmem_spec, vmem_spec],
            out_specs=(any_spec, any_spec, any_spec, any_spec),
            scratch_shapes=[pltpu.SMEM((1, 1), F32), pltpu.SMEM((1, 1), F32), dma((4,))],
            compiler_params=pltpu.CompilerParams(vmem_limit_bytes=MARGIN),
            name="put_rows",
        )(scalars, d_img, d_txt)
        return loss.reshape(()), d_img, d_txt, d_scale.reshape(())

    return jax.shard_map(local_tile, mesh=mesh, in_specs=(batch_spec, batch_spec, P()), out_specs=(P(), batch_spec, batch_spec, P()), check_vma=False)
```
